768 devices in a mesh: space: 24 (over x, z_lo), batch: 32 (over z_hi, y, core).
Axes of the slice: x: 4, y: 8, z: 12 (z_hi: 2, z_lo: 6; z = z_hi * 6 + z_lo), core: 2. Of those that a mesh axis runs over, the one named last changes fastest.
Arguments:
- pre_act: bfloat16 [32, 64, 24, 8, 128], P('batch', None, 'space'), may hold values from -6 to 6
- grad_out: bfloat16 [32, 128, 24, 8, 128], P('batch', None, 'space'), may hold values from -6 to 6
- weight: bfloat16 [27, 64, 128], replicated, may hold values from -0.109375 to 0.109375
Outputs:
- grad_in: bfloat16 [32, 64, 24, 8, 128], P('batch', None, 'space')
- weight_grad: float32 [221184], P(('space', 'batch'))
The draws below stay inside these ranges and needn't reach their ends.
All inputs are finite; a program needn't handle non-finite values.
Results may differ from the reference program's by a relative error of at most 0.001.
Values may be sent and summed in bfloat16 or wider, within the bound.
No kernel may reach another device: no remote copies, remote signals or barrier semaphores. Data moves between devices by JAX's collectives and lax.ppermute only.
A program may use at most 32 MiB of HBM per device.

```python
import jax
import jax.numpy as jnp
from jax import lax

CIN = 64
COUT = 128
YC = 8
ZC = 128
SAMPLES = 32
NX = 24


def block_scale(stream_key, dims, pieces, least, high):
    loudness, own = 1.0, jax.random.fold_in(stream_key, 6)
    for dim, shards_of in pieces:
        draws = jnp.exp(jax.random.uniform(jax.random.fold_in(own, dim), (shards_of,), jnp.float32, least / len(pieces), high / len(pieces)))
        loudness = loudness * jnp.repeat(draws, dims[dim] // shards_of).reshape([-1 if axis == dim else 1 for axis in range(len(dims))])
    return loudness


def normal_values(key, extent, scale, most, pieces=(), dtype=jnp.bfloat16):
    values = jax.random.normal(key, extent, jnp.float32) * scale
    if len(pieces) > 0:
        values = block_scale(key, extent, pieces, -0.22, 0.18) * values
    return jnp.clip(values, min=-most, max=most).astype(dtype)


def setup_inputs(seed: int = 0) -> dict:
    key_list = jax.random.split(jax.random.key(seed), 4)
    return {
        "pre_act": normal_values(key_list[0], (SAMPLES, CIN, NX, YC, ZC), 1.0, 6.0, ((0, 32), (2, 24))),
        "grad_out": normal_values(key_list[1], (SAMPLES, COUT, NX, YC, ZC), 1.0, 6.0, ((0, 32), (2, 24))),
        "weight": normal_values(key_list[2], (27, CIN, COUT), (27 * COUT) ** -0.5, 0.109375),
    }


slope = 0.3

def reference(pre_act, grad_out, weight):
    factor = 1.0 / jnp.sqrt(jnp.float32(SAMPLES * NX * YC * ZC))
    kernel = weight.astype(jnp.float32)

    def per_sample(sample_pair):
        act_one, grad_one = sample_pair
        act_float = act_one.astype(jnp.float32)
        hidden = jnp.where(act_float > 0, act_float, slope * act_float).astype(jnp.bfloat16)
        hidden = lax.optimization_barrier(hidden).astype(jnp.float32)
        padded = jnp.pad(grad_one.astype(jnp.float32), ((0, 0), (1, 1), (1, 1), (1, 1)))
        grad_hidden = jnp.zeros((CIN, NX, YC, ZC), jnp.float32)
        tap_grads = []
        for tap in range(27):
            shift_x = tap // 9 - 1
            shift_y = tap // 3 % 3 - 1
            shift_z = tap % 3 - 1
            window = padded[:, 1 - shift_x:1 - shift_x + NX, 1 - shift_y:1 - shift_y + YC, 1 - shift_z:1 - shift_z + ZC]
            grad_hidden = grad_hidden + jnp.einsum('ic,cxyz->ixyz', kernel[tap], window, precision=lax.Precision.HIGHEST)
            tap_grads.append(jnp.einsum('ixyz,cxyz->ic', hidden, window, precision=lax.Precision.HIGHEST))
        grad_one_in = (grad_hidden * jnp.where(act_float > 0, 1.0, slope)).astype(jnp.bfloat16)
        return (grad_one_in, jnp.stack(tap_grads))
    grad_in, taps_all = lax.map(per_sample, (pre_act, grad_out))
    weight_grad = (lax.optimization_barrier(jnp.sum(taps_all, axis=0)) * factor).reshape(-1)
    return (grad_in, weight_grad)
```

```python
import functools

import jax
import jax.numpy as jnp
from jax import lax
from jax.experimental import pallas as pl
from jax.experimental.pallas import tpu as pltpu
from jax.sharding import PartitionSpec as P

slope = 0.3
CIN, COUT, YC, ZC, TAPS = 64, 128, 8, 128, 27
ROWS = TAPS * CIN
TOP = 12.0


def shifted_lanes(tile, by):
    lane = lax.broadcasted_iota(jnp.int32, tile.shape, 1)
    if by > 0:
        return jnp.where(lane > 0, pltpu.roll(tile, 1, 1), 0.0)
    return jnp.where(lane < ZC - 1, pltpu.roll(tile, ZC - 1, 1), 0.0)


def kernel(factor, act_ref, own_ref, low_ref, high_ref, w_ref, gin_ref, wg_ref, exp_ref, wide, acts, grads, hids):
    for plane, (u, ref) in enumerate(((-1, high_ref), (0, own_ref), (1, low_ref))):
        wide[...] = ref[...].astype(jnp.float32).reshape(COUT * YC, ZC)
        for y in range(YC):
            tile = wide[pl.ds(y, COUT, stride=YC), :]
            for w in (-1, 0, 1):
                moved = tile if w == 0 else shifted_lanes(tile, w)
                row = (plane * 3 + w + 1) * COUT
                grads[row : row + COUT, y * ZC : (y + 1) * ZC] = moved.astype(jnp.bfloat16)
    act = act_ref[...].astype(jnp.float32)
    hidden = jnp.where(act > 0, act, slope * act).astype(jnp.bfloat16)
    acts[...] = hidden.astype(jnp.float32).reshape(CIN * YC, ZC)
    for y in range(YC):
        tile = acts[pl.ds(y, CIN, stride=YC), :].astype(jnp.bfloat16)
        for v in (-1, 0, 1):
            if 0 <= y - v < YC:
                hids[(v + 1) * CIN : (v + 2) * CIN, (y - v) * ZC : (y - v + 1) * ZC] = tile
    none = jnp.zeros((CIN, ZC), jnp.bfloat16)
    hids[0:CIN, 0:ZC] = none
    hids[2 * CIN : 3 * CIN, (YC - 1) * ZC : YC * ZC] = none

    taps = lax.dot_general(
        hids[...], grads[...], (((1,), (1,)), ((), ())), preferred_element_type=jnp.float32
    )
    most = jnp.max(jnp.abs(taps), keepdims=True) * factor
    exponent = jnp.floor(jnp.log2(jnp.maximum(most, 1e-36))) + 1.0
    exp_ref[...] = jnp.broadcast_to(exponent, exp_ref.shape)
    scale = jnp.broadcast_to(jnp.exp2(TOP - exponent) * factor, (CIN, COUT))
    for u in range(3):
        for v in range(3):
            for w in range(3):
                tap = 9 * u + 3 * v + w
                block = taps[v * CIN : (v + 1) * CIN, (u * 3 + w) * COUT : (u * 3 + w + 1) * COUT]
                wg_ref[tap * CIN : (tap + 1) * CIN, :] = (block * scale).astype(wg_ref.dtype)

    weights = jnp.concatenate(
        [
            jnp.concatenate([w_ref[9 * u + 3 * v + w] for u in range(3) for w in range(3)], axis=1)
            for v in range(3)
        ],
        axis=0,
    )
    sums = lax.dot_general(
        weights, grads[...], (((1,), (0,)), ((), ())), preferred_element_type=jnp.float32
    )
    for y in range(YC):
        total = sums[CIN : 2 * CIN, y * ZC : (y + 1) * ZC]
        if y + 1 < YC:
            total = total + sums[0:CIN, (y + 1) * ZC : (y + 2) * ZC]
        if y - 1 >= 0:
            total = total + sums[2 * CIN : 3 * CIN, (y - 1) * ZC : y * ZC]
        acts[pl.ds(y, CIN, stride=YC), :] = total
    grad_hidden = acts[...].reshape(CIN, YC, ZC)
    gin_ref[...] = (grad_hidden * jnp.where(act > 0, 1.0, slope)).astype(jnp.bfloat16)


def local_grads(factor, act, own, low, high, weight, wg_dtype):
    return pl.pallas_call(
        functools.partial(kernel, factor),
        out_shape=(
            jax.ShapeDtypeStruct((CIN, YC, ZC), jnp.bfloat16),
            jax.ShapeDtypeStruct((ROWS, COUT), wg_dtype),
            jax.ShapeDtypeStruct((8, 128), jnp.float32),
        ),
        in_specs=[pl.BlockSpec(memory_space=pltpu.VMEM)] * 5,
        out_specs=tuple([pl.BlockSpec(memory_space=pltpu.VMEM)] * 3),
        scratch_shapes=[
            pltpu.VMEM((COUT * YC, ZC), jnp.float32),
            pltpu.VMEM((CIN * YC, ZC), jnp.float32),
            pltpu.VMEM((9 * COUT, YC * ZC), jnp.bfloat16),
            pltpu.VMEM((3 * CIN, YC * ZC), jnp.bfloat16),
        ],
        compiler_params=pltpu.CompilerParams(vmem_limit_bytes=20 * 1024 * 1024),
        cost_estimate=pl.CostEstimate(flops=900_000_000, bytes_accessed=2_500_000, transcendentals=0),
        name="local_grads",
    )(act, own, low, high, weight)


XS, ZL, ZH, YS, CS = 4, 6, 2, 8, 2


def device(x, zl, zh, y, c):
    return (x * ZL + zl) * ZH * YS * CS + zh * YS * CS + y * CS + c


def groups():
    along_x = [[x * ZL + zl for x in range(XS)] for zl in range(ZL)]
    along_z = [
        [device(x, zl, zh, y, c) for zl in range(ZL) for zh in range(ZH)]
        for x in range(XS)
        for y in range(YS)
        for c in range(CS)
    ]
    along_y = [[zh * YS * CS + i for i in range(YS * CS)] for zh in range(ZH)]
    return along_x, along_z, along_y


def coded(scaled, exponent):
    mark = jnp.broadcast_to(exponent, (scaled.shape[0], 16, 128)).astype(jnp.float16)
    return jnp.concatenate([scaled.astype(jnp.float16), mark], axis=1)


def on_device(pre_act, grad_out, weight):
    count = pre_act.shape[0] * 32 * pre_act.shape[2] * 24 * YC * ZC
    factor = float(1.0 / count**0.5)
    steps = lax.axis_size("space")
    forward = [(i, i + 1) for i in range(steps - 1)]
    backward = [(i + 1, i) for i in range(steps - 1)]
    own = grad_out.reshape(COUT, YC, ZC)
    low = lax.ppermute(own, "space", forward)
    high = lax.ppermute(own, "space", backward)
    grad_in, partial, exponent = local_grads(
        factor, pre_act.reshape(CIN, YC, ZC), own, low, high, weight, jnp.float32
    )
    along_x, along_z, along_y = groups()
    rows = ROWS // XS
    sent = coded(partial.reshape(XS, rows, COUT), exponent[0, 0])
    got = lax.all_to_all(sent, "space", 0, 0, tiled=True, axis_index_groups=along_x)
    exps = got[:, rows, 0].astype(jnp.float32)
    largest = jnp.max(exps) + 2.0
    weights = jnp.exp2(exps - largest)
    part = jnp.sum(got[:, :rows].astype(jnp.float32) * weights[:, None, None], axis=0)
    rows = rows // (ZL * ZH)
    sent = coded(part.reshape(ZL * ZH, rows, COUT), largest)
    got = lax.all_to_all(sent, ("space", "batch"), 0, 0, tiled=True, axis_index_groups=along_z)
    weights = jnp.exp2(got[:, rows, 0].astype(jnp.float32) - TOP)
    part = jnp.sum(got[:, :rows].astype(jnp.float32) * weights[:, None, None], axis=0)
    sent = part.reshape(YS * CS, rows * COUT // (YS * CS))
    got = lax.all_to_all(sent, "batch", 0, 0, tiled=True, axis_index_groups=along_y)
    weight_grad = jnp.sum(got, axis=0)
    return (grad_in.reshape(pre_act.shape), weight_grad)


def solution(mesh):
    return jax.shard_map(
        on_device,
        mesh=mesh,
        in_specs=(
            P("batch", None, "space", None, None),
            P("batch", None, "space", None, None),
            P(),
        ),
        out_specs=(P("batch", None, "space", None, None), P(("space", "batch"))),
        check_vma=False,
    )
```

```python
import functools

import jax
import jax.numpy as jnp
from jax import lax
from jax.experimental import pallas as pl
from jax.experimental.pallas import tpu as pltpu
from jax.sharding import PartitionSpec as P

slope = 0.3
CIN, COUT, YC, ZC, TAPS = 64, 128, 8, 128, 27
CELLS = YC * ZC
ROWS = TAPS * CIN
XS, ZL, ZH, YS, CS = 4, 6, 2, 8, 2
ZS, YCS = ZL * ZH, YS * CS
XROWS = ROWS // XS
ZROWS = XROWS // ZS
PART = 3
MARKS = 16
TOP = 12.0


def shifted_lanes(tile, by):
    lane = lax.broadcasted_iota(jnp.int32, tile.shape, 1)
    if by > 0:
        return jnp.where(lane > 0, pltpu.roll(tile, 1, 1), 0.0)
    return jnp.where(lane < ZC - 1, pltpu.roll(tile, ZC - 1, 1), 0.0)


def spread(ref, wide, grads, first):
    wide[...] = ref[...].astype(jnp.float32).reshape(COUT * YC, ZC)
    for y in range(YC):
        tile = wide[pl.ds(y, COUT, stride=YC), :]
        for w in (-1, 0, 1):
            moved = tile if w == 0 else shifted_lanes(tile, w)
            row = first + (w + 1) * COUT
            grads[row : row + COUT, y * ZC : (y + 1) * ZC] = moved.astype(jnp.bfloat16)


def by_taps(hids, grads):
    return lax.dot_general(
        hids[...], grads[...], (((1,), (1,)), ((), ())), preferred_element_type=jnp.float32
    )


def by_cells(weights, grads):
    return lax.dot_general(
        weights[...], grads[...], (((1,), (0,)), ((), ())), preferred_element_type=jnp.float32
    )


def own_kernel(act_ref, own_ref, w_ref, hid_ref, tap_ref, sum_ref, side_ref, wide, acts, grads, mids):
    spread(own_ref, wide, grads, 0)
    act = act_ref[...].astype(jnp.float32)
    hidden = jnp.where(act > 0, act, slope * act).astype(jnp.bfloat16)
    acts[...] = hidden.astype(jnp.float32).reshape(CIN * YC, ZC)
    for y in range(YC):
        tile = acts[pl.ds(y, CIN, stride=YC), :].astype(jnp.bfloat16)
        for v in (-1, 0, 1):
            if 0 <= y - v < YC:
                hid_ref[(v + 1) * CIN : (v + 2) * CIN, (y - v) * ZC : (y - v + 1) * ZC] = tile
    none = jnp.zeros((CIN, ZC), jnp.bfloat16)
    hid_ref[0:CIN, 0:ZC] = none
    hid_ref[2 * CIN : 3 * CIN, (YC - 1) * ZC : YC * ZC] = none
    for v in range(3):
        for w in range(3):
            rows, lanes = slice(v * CIN, (v + 1) * CIN), slice(w * COUT, (w + 1) * COUT)
            mids[rows, lanes] = w_ref[9 + 3 * v + w]
            side_ref[rows, lanes] = w_ref[3 * v + w]
            side_ref[rows, (w + 3) * COUT : (w + 4) * COUT] = w_ref[18 + 3 * v + w]
    tap_ref[...] = by_taps(hid_ref, grads)
    sum_ref[...] = by_cells(mids, grads)


def side_kernel(
    factor, act_ref, low_ref, high_ref, hid_ref, tap_ref, sum_ref, side_ref, sent_ref, gin_ref, wide, acts, grads
):
    spread(high_ref, wide, grads, 0)
    spread(low_ref, wide, grads, 3 * COUT)
    outer = by_taps(hid_ref, grads)
    inner = tap_ref[...]
    most = jnp.maximum(
        jnp.max(jnp.abs(outer), keepdims=True), jnp.max(jnp.abs(inner), keepdims=True)
    )
    exponent = jnp.floor(jnp.log2(jnp.maximum(most * factor, 1e-30))) + 1.0
    scale = jnp.broadcast_to(jnp.exp2(TOP - exponent) * factor, (CIN, COUT))
    for x in range(XS):
        sent_ref[x, XROWS : XROWS + MARKS, :] = jnp.broadcast_to(exponent, (MARKS, COUT))
    for tap in range(TAPS):
        u, v, w = tap // 9, tap // 3 % 3, tap % 3
        rows = slice(v * CIN, (v + 1) * CIN)
        if u == 1:
            block = inner[rows, w * COUT : (w + 1) * COUT]
        else:
            lane = (u // 2 * 3 + w) * COUT
            block = outer[rows, lane : lane + COUT]
        block = block * scale
        first = tap * CIN
        while first < (tap + 1) * CIN:
            x = first // XROWS
            last = min((tap + 1) * CIN, (x + 1) * XROWS)
            sent_ref[x, first - x * XROWS : last - x * XROWS, :] = block[first - tap * CIN : last - tap * CIN]
            first = last
    sums = by_cells(side_ref, grads) + sum_ref[...]
    for y in range(YC):
        total = sums[CIN : 2 * CIN, y * ZC : (y + 1) * ZC]
        if y + 1 < YC:
            total = total + sums[0:CIN, (y + 1) * ZC : (y + 2) * ZC]
        if y - 1 >= 0:
            total = total + sums[2 * CIN : 3 * CIN, (y - 1) * ZC : y * ZC]
        acts[pl.ds(y, CIN, stride=YC), :] = total
    grad_hidden = acts[...].reshape(CIN, YC, ZC)
    act = act_ref[...].astype(jnp.float32)
    gin_ref[...] = (grad_hidden * jnp.where(act > 0, 1.0, slope)).astype(jnp.bfloat16)


def after_x_kernel(got_ref, sent_ref, total):
    exps = [got_ref[i, XROWS : XROWS + 1, :] for i in range(XS)]
    largest = functools.reduce(jnp.maximum, exps) + 2.0
    total[...] = sum(got_ref[i, 0:XROWS, :] * jnp.exp2(exps[i] - largest) for i in range(XS))
    for part in range(YCS):
        row = 9 * (part // 4) + 2 * (part % 4)
        for i in range(PART):
            sent_ref[part, i * ZS : (i + 1) * ZS, :] = total[pl.ds(row + i, ZS, stride=ZROWS), :]
        sent_ref[part, PART * ZS : PART * ZS + 12, :] = jnp.broadcast_to(largest, (12, COUT))


def after_y_kernel(got_ref, sent_ref):
    total = jnp.zeros((PART * ZS, COUT), jnp.float32)
    for i in range(YCS):
        weight = jnp.exp2(got_ref[i, PART * ZS : PART * ZS + 1, :] - TOP)
        total = total + got_ref[i, 0 : PART * ZS, :] * weight
    for i in range(PART):
        sent_ref[:, i, :] = total[i * ZS : (i + 1) * ZS]


def call(body, name, outs, scratch, flops, *args):
    vmem = pl.BlockSpec(memory_space=pltpu.VMEM)
    return pl.pallas_call(
        body,
        out_shape=tuple(jax.ShapeDtypeStruct(shape, dtype) for shape, dtype in outs),
        in_specs=[vmem] * len(args),
        out_specs=tuple([vmem] * len(outs)),
        scratch_shapes=[pltpu.VMEM(shape, dtype) for shape, dtype in scratch],
        compiler_params=pltpu.CompilerParams(vmem_limit_bytes=16 * 1024 * 1024),
        cost_estimate=pl.CostEstimate(flops=flops, bytes_accessed=2_000_000, transcendentals=0),
        name=name,
    )(*args)


def device(x, zl, zh, y, c):
    return (x * ZL + zl) * ZH * YCS + zh * YCS + y * CS + c


def groups():
    along_x = [[x * ZL + zl for x in range(XS)] for zl in range(ZL)]
    along_y = [[zh * YCS + i for i in range(YCS)] for zh in range(ZH)]
    along_z = [
        [device(x, zl, zh, y, c) for zl in range(ZL) for zh in range(ZH)]
        for x in range(XS)
        for y in range(YS)
        for c in range(CS)
    ]
    return along_x, along_y, along_z


def exchanged(x, axis, members):
    return lax.all_to_all(x, axis, 0, 0, tiled=True, axis_index_groups=members)


def on_device(pre_act, grad_out, weight):
    f32, bf16, f16 = jnp.float32, jnp.bfloat16, jnp.float16
    count = pre_act.shape[0] * lax.axis_size("batch") * lax.axis_size("space") * CELLS
    factor = float(1.0 / count**0.5)
    steps = lax.axis_size("space")
    forward = [(i, i + 1) for i in range(steps - 1)]
    backward = [(i + 1, i) for i in range(steps - 1)]
    along_x, along_y, along_z = groups()

    act = pre_act.reshape(CIN, YC, ZC)
    own = grad_out.reshape(COUT, YC, ZC)
    low = lax.ppermute(own, "space", forward)
    high = lax.ppermute(own, "space", backward)
    plane = ((COUT * YC, ZC), f32)
    small = ((CIN * YC, ZC), f32)
    hids, taps, sums, sides = call(
        own_kernel,
        "own_plane",
        [((3 * CIN, CELLS), bf16), ((3 * CIN, 3 * COUT), f32), ((3 * CIN, CELLS), f32), ((3 * CIN, 6 * COUT), bf16)],
        [plane, small, ((3 * COUT, CELLS), bf16), ((3 * CIN, 3 * COUT), bf16)],
        1_000_000_000,
        act, own, weight,
    )
    sent, grad_in = call(
        functools.partial(side_kernel, factor),
        "side_planes",
        [((XS, XROWS + MARKS, COUT), f32), ((CIN, YC, ZC), bf16)],
        [plane, small, ((6 * COUT, CELLS), bf16)],
        2_000_000_000,
        act, low, high, hids, taps, sums, sides,
    )
    got = exchanged(sent.astype(f16), "space", along_x).astype(f32)
    (sent,) = call(
        after_x_kernel, "after_x", [((YCS, PART * ZS + 12, COUT), f32)], [((XROWS, COUT), f32)], 1_000_000, got
    )
    got = exchanged(sent.astype(f16), "batch", along_y).astype(f32)
    (sent,) = call(after_y_kernel, "after_y", [((ZS, PART, COUT), f32)], [], 1_000_000, got)
    got = exchanged(sent, ("space", "batch"), along_z)
    total = jnp.sum(got, axis=0).reshape(-1)
    start = (lax.axis_index("batch") & 3) * 32
    weight_grad = lax.dynamic_slice(total, (start,), (ROWS * COUT // 768,))
    return (grad_in.reshape(pre_act.shape), weight_grad)


def solution(mesh):
    return jax.shard_map(
        on_device,
        mesh=mesh,
        in_specs=(
            P("batch", None, "space", None, None),
            P("batch", None, "space", None, None),
            P(),
        ),
        out_specs=(P("batch", None, "space", None, None), P(("space", "batch"))),
        check_vma=False,
    )
```

```python
import functools

import jax
import jax.numpy as jnp
from jax import lax
from jax.experimental import pallas as pl
from jax.experimental.pallas import tpu as pltpu
from jax.sharding import PartitionSpec as P

slope = 0.3
CIN, COUT, YC, ZC, TAPS = 64, 128, 8, 128, 27
CELLS = YC * ZC
ROWS = TAPS * CIN
XS, ZL, ZH, YS, CS = 4, 6, 2, 8, 2
ZS, YCS = ZL * ZH, YS * CS
XROWS = ROWS // XS
ZROWS = XROWS // ZS
PART = 3
XMARKS, YMARKS = 8, 4
TOP = 12.0


def shifted_lanes(tile, by):
    lane = lax.broadcasted_iota(jnp.int32, tile.shape, 1)
    if by > 0:
        return jnp.where(lane > 0, pltpu.roll(tile, 1, 1), 0.0)
    return jnp.where(lane < ZC - 1, pltpu.roll(tile, ZC - 1, 1), 0.0)


def spread(ref, wide, grads, first):
    wide[...] = ref[...].astype(jnp.float32).reshape(COUT * YC, ZC)
    for y in range(YC):
        tile = wide[pl.ds(y, COUT, stride=YC), :]
        for w in (-1, 0, 1):
            moved = tile if w == 0 else shifted_lanes(tile, w)
            row = first + (w + 1) * COUT
            grads[row : row + COUT, y * ZC : (y + 1) * ZC] = moved.astype(jnp.bfloat16)


def by_taps(hids, grads):
    return lax.dot_general(
        hids[...], grads[...], (((1,), (1,)), ((), ())), preferred_element_type=jnp.float32
    )


def by_cells(weights, grads):
    return lax.dot_general(
        weights[...], grads[...], (((1,), (0,)), ((), ())), preferred_element_type=jnp.float32
    )


def stack_hidden(act, acts, hids):
    hidden = jnp.where(act > 0, act, slope * act).astype(jnp.bfloat16)
    acts[...] = hidden.astype(jnp.float32).reshape(CIN * YC, ZC)
    for y in range(YC):
        tile = acts[pl.ds(y, CIN, stride=YC), :].astype(jnp.bfloat16)
        for v in (-1, 0, 1):
            if 0 <= y - v < YC:
                hids[(v + 1) * CIN : (v + 2) * CIN, (y - v) * ZC : (y - v + 1) * ZC] = tile
    none = jnp.zeros((CIN, ZC), jnp.bfloat16)
    hids[0:CIN, 0:ZC] = none
    hids[2 * CIN : 3 * CIN, (YC - 1) * ZC : YC * ZC] = none


def own_kernel(
    act_ref, own_ref, w_ref, hid_ref, grad_ref, tap_ref, sum_ref, up_ref, down_ref, wide, acts, mids
):
    spread(own_ref, wide, grad_ref, 0)
    stack_hidden(act_ref[...].astype(jnp.float32), acts, hid_ref)
    for v in range(3):
        for w in range(3):
            rows, lanes = slice(v * CIN, (v + 1) * CIN), slice(w * COUT, (w + 1) * COUT)
            down_ref[rows, lanes] = w_ref[3 * v + w]
            mids[rows, lanes] = w_ref[9 + 3 * v + w]
            up_ref[rows, lanes] = w_ref[18 + 3 * v + w]
    tap_ref[...] = by_taps(hid_ref, grad_ref)
    sum_ref[...] = by_cells(mids, grad_ref)


def side_kernel(
    factor, act_ref, low_ref, hid_ref, grad_ref, tap_ref, sent_ref, moved_ref, wide, acts, hids
):
    spread(low_ref, wide, moved_ref, 0)
    stack_hidden(act_ref[...].astype(jnp.float32), acts, hids)
    taps = (by_taps(hids, grad_ref), tap_ref[...], by_taps(hid_ref, moved_ref))
    most = functools.reduce(jnp.maximum, [jnp.max(jnp.abs(t), keepdims=True) for t in taps])
    exponent = jnp.floor(jnp.log2(jnp.maximum(most * factor, 1e-30))) + 1.0
    scale = jnp.broadcast_to(jnp.exp2(TOP - exponent) * factor, (CIN, COUT))
    for x in range(XS):
        sent_ref[x, XROWS : XROWS + XMARKS, :] = jnp.broadcast_to(exponent, (XMARKS, COUT))
    for tap in range(TAPS):
        u, v, w = tap // 9, tap // 3 % 3, tap % 3
        block = taps[u][v * CIN : (v + 1) * CIN, w * COUT : (w + 1) * COUT] * scale
        first = tap * CIN
        while first < (tap + 1) * CIN:
            x = first // XROWS
            last = min((tap + 1) * CIN, (x + 1) * XROWS)
            sent_ref[x, first - x * XROWS : last - x * XROWS, :] = block[first - tap * CIN : last - tap * CIN]
            first = last


def grad_kernel(act_ref, high_ref, moved_ref, sum_ref, up_ref, down_ref, gin_ref, wide, acts, grads):
    spread(high_ref, wide, grads, 0)
    sums = by_cells(down_ref, grads) + by_cells(up_ref, moved_ref) + sum_ref[...]
    for y in range(YC):
        total = sums[CIN : 2 * CIN, y * ZC : (y + 1) * ZC]
        if y + 1 < YC:
            total = total + sums[0:CIN, (y + 1) * ZC : (y + 2) * ZC]
        if y - 1 >= 0:
            total = total + sums[2 * CIN : 3 * CIN, (y - 1) * ZC : y * ZC]
        acts[pl.ds(y, CIN, stride=YC), :] = total
    grad_hidden = acts[...].reshape(CIN, YC, ZC)
    act = act_ref[...].astype(jnp.float32)
    gin_ref[...] = (grad_hidden * jnp.where(act > 0, 1.0, slope)).astype(jnp.bfloat16)


def after_x_kernel(got_ref, sent_ref, total):
    exps = [got_ref[i, XROWS : XROWS + 1, :] for i in range(XS)]
    largest = functools.reduce(jnp.maximum, exps) + 2.0
    total[...] = sum(got_ref[i, 0:XROWS, :] * jnp.exp2(exps[i] - largest) for i in range(XS))
    for part in range(YCS):
        row = 9 * (part // 4) + 2 * (part % 4)
        for i in range(PART):
            sent_ref[part, i * ZS : (i + 1) * ZS, :] = total[pl.ds(row + i, ZS, stride=ZROWS), :]
        sent_ref[part, PART * ZS : PART * ZS + YMARKS, :] = jnp.broadcast_to(largest, (YMARKS, COUT))


def after_y_kernel(got_ref, sent_ref):
    total = jnp.zeros((PART * ZS, COUT), jnp.float32)
    for i in range(YCS):
        weight = jnp.exp2(got_ref[i, PART * ZS : PART * ZS + 1, :] - TOP)
        total = total + got_ref[i, 0 : PART * ZS, :] * weight
    for i in range(PART):
        sent_ref[:, i, :] = total[i * ZS : (i + 1) * ZS]


def call(body, name, outs, scratch, flops, *args):
    vmem = pl.BlockSpec(memory_space=pltpu.VMEM)
    return pl.pallas_call(
        body,
        out_shape=tuple(jax.ShapeDtypeStruct(shape, dtype) for shape, dtype in outs),
        in_specs=[vmem] * len(args),
        out_specs=tuple([vmem] * len(outs)),
        scratch_shapes=[pltpu.VMEM(shape, dtype) for shape, dtype in scratch],
        compiler_params=pltpu.CompilerParams(vmem_limit_bytes=16 * 1024 * 1024),
        cost_estimate=pl.CostEstimate(flops=flops, bytes_accessed=2_000_000, transcendentals=0),
        name=name,
    )(*args)


def device(x, zl, zh, y, c):
    return (x * ZL + zl) * ZH * YCS + zh * YCS + y * CS + c


def groups():
    along_x = [[x * ZL + zl for x in range(XS)] for zl in range(ZL)]
    along_y = [[zh * YCS + i for i in range(YCS)] for zh in range(ZH)]
    along_z = [
        [device(x, zl, zh, y, c) for zl in range(ZL) for zh in range(ZH)]
        for x in range(XS)
        for y in range(YS)
        for c in range(CS)
    ]
    return along_x, along_y, along_z


def exchanged(x, axis, members):
    return lax.all_to_all(x, axis, 0, 0, tiled=True, axis_index_groups=members)


def on_device(pre_act, grad_out, weight):
    f32, bf16, f16 = jnp.float32, jnp.bfloat16, jnp.float16
    count = pre_act.shape[0] * lax.axis_size("batch") * lax.axis_size("space") * CELLS
    factor = float(1.0 / count**0.5)
    steps = lax.axis_size("space")
    forward = [(i, i + 1) for i in range(steps - 1)]
    backward = [(i + 1, i) for i in range(steps - 1)]
    along_x, along_y, along_z = groups()

    act = pre_act.reshape(CIN, YC, ZC)
    own = grad_out.reshape(COUT, YC, ZC)
    low = lax.ppermute(own, "space", forward)
    low_act = lax.ppermute(act, "space", forward)
    plane = ((COUT * YC, ZC), f32)
    small = ((CIN * YC, ZC), f32)
    stacked, moved, third = ((3 * CIN, CELLS), bf16), ((3 * COUT, CELLS), bf16), ((3 * CIN, 3 * COUT), bf16)
    hids, grads, taps, sums, up, down = call(
        own_kernel,
        "own_plane",
        [stacked, moved, ((3 * CIN, 3 * COUT), f32), ((3 * CIN, CELLS), f32), third, third],
        [plane, small, third],
        1_000_000_000,
        act, own, weight,
    )
    sent, low_grads = call(
        functools.partial(side_kernel, factor),
        "side_planes",
        [((XS, XROWS + XMARKS, COUT), f32), moved],
        [plane, small, stacked],
        1_000_000_000,
        low_act, low, hids, grads, taps,
    )
    got = exchanged(sent.astype(f16), "space", along_x).astype(f32)
    (sent,) = call(
        after_x_kernel, "after_x", [((YCS, PART * ZS + YMARKS, COUT), f32)], [((XROWS, COUT), f32)], 1_000_000, got
    )
    own, sent = lax.optimization_barrier((own, sent))
    high = lax.ppermute(own, "space", backward)
    got = exchanged(sent.astype(f16), "batch", along_y).astype(f32)
    (sent,) = call(after_y_kernel, "after_y", [((ZS, PART, COUT), f32)], [], 1_000_000, got)
    high, sent = lax.optimization_barrier((high, sent))
    (grad_in,) = call(
        grad_kernel,
        "grad_planes",
        [((CIN, YC, ZC), bf16)],
        [plane, small, moved],
        2_000_000_000,
        act, high, low_grads, sums, up, down,
    )
    got = exchanged(sent, ("space", "batch"), along_z)
    total = jnp.sum(got, axis=0).reshape(-1)
    start = (lax.axis_index("batch") & 3) * 32
    weight_grad = lax.dynamic_slice(total, (start,), (ROWS * COUT // 768,))
    return (grad_in.reshape(pre_act.shape), weight_grad)


def solution(mesh):
    return jax.shard_map(
        on_device,
        mesh=mesh,
        in_specs=(
            P("batch", None, "space", None, None),
            P("batch", None, "space", None, None),
            P(),
        ),
        out_specs=(P("batch", None, "space", None, None), P(("space", "batch"))),
        check_vma=False,
    )
```

```python
import functools

import jax
import jax.numpy as jnp
from jax import lax
from jax.experimental import pallas as pl
from jax.experimental.pallas import tpu as pltpu
from jax.sharding import PartitionSpec as P

slope = 0.3
CIN, COUT, YC, ZC, TAPS = 64, 128, 8, 128, 27
CELLS = YC * ZC
ROWS = TAPS * CIN
XS, ZL, ZH, YS, CS = 4, 6, 2, 8, 2
ZS, YCS = ZL * ZH, YS * CS
XROWS = ROWS // XS
ZROWS = XROWS // ZS
PART = 3
XMARKS, YMARKS = 8, 4
TOP = 12.0


def shifted_lanes(tile, by):
    lane = lax.broadcasted_iota(jnp.int32, tile.shape, 1)
    if by > 0:
        return jnp.where(lane > 0, pltpu.roll(tile, 1, 1), 0.0)
    return jnp.where(lane < ZC - 1, pltpu.roll(tile, ZC - 1, 1), 0.0)


def spread(ref, wide, grads, first):
    wide[...] = ref[...].astype(jnp.float32).reshape(COUT * YC, ZC)
    for y in range(YC):
        tile = wide[pl.ds(y, COUT, stride=YC), :]
        for w in (-1, 0, 1):
            moved = tile if w == 0 else shifted_lanes(tile, w)
            row = first + (w + 1) * COUT
            grads[row : row + COUT, y * ZC : (y + 1) * ZC] = moved.astype(jnp.bfloat16)


def by_taps(hids, grads):
    return lax.dot_general(
        hids[...], grads[...], (((1,), (1,)), ((), ())), preferred_element_type=jnp.float32
    )


def by_cells(weights, grads):
    return lax.dot_general(
        weights[...], grads[...], (((1,), (0,)), ((), ())), preferred_element_type=jnp.float32
    )


def stack_hidden(act, acts, hids):
    hidden = jnp.where(act > 0, act, slope * act).astype(jnp.bfloat16)
    acts[...] = hidden.astype(jnp.float32).reshape(CIN * YC, ZC)
    for y in range(YC):
        tile = acts[pl.ds(y, CIN, stride=YC), :].astype(jnp.bfloat16)
        for v in (-1, 0, 1):
            if 0 <= y - v < YC:
                hids[(v + 1) * CIN : (v + 2) * CIN, (y - v) * ZC : (y - v + 1) * ZC] = tile
    none = jnp.zeros((CIN, ZC), jnp.bfloat16)
    hids[0:CIN, 0:ZC] = none
    hids[2 * CIN : 3 * CIN, (YC - 1) * ZC : YC * ZC] = none


def own_kernel(
    act_ref, own_ref, w_ref, hid_ref, grad_ref, tap_ref, sum_ref, up_ref, down_ref, wide, acts, mids
):
    spread(own_ref, wide, grad_ref, 0)
    stack_hidden(act_ref[...].astype(jnp.float32), acts, hid_ref)
    for v in range(3):
        for w in range(3):
            rows, lanes = slice(v * CIN, (v + 1) * CIN), slice(w * COUT, (w + 1) * COUT)
            down_ref[rows, lanes] = w_ref[3 * v + w]
            mids[rows, lanes] = w_ref[9 + 3 * v + w]
            up_ref[rows, lanes] = w_ref[18 + 3 * v + w]
    tap_ref[...] = by_taps(hid_ref, grad_ref)
    sum_ref[...] = by_cells(mids, grad_ref)


def side_kernel(
    factor, act_ref, low_ref, hid_ref, grad_ref, tap_ref, sent_ref, moved_ref, wide, acts, hids
):
    spread(low_ref, wide, moved_ref, 0)
    stack_hidden(act_ref[...].astype(jnp.float32), acts, hids)
    taps = (by_taps(hids, grad_ref), tap_ref[...], by_taps(hid_ref, moved_ref))
    most = functools.reduce(jnp.maximum, [jnp.max(jnp.abs(t), keepdims=True) for t in taps])
    exponent = jnp.floor(jnp.log2(jnp.maximum(most * factor, 1e-30))) + 1.0
    scale = jnp.broadcast_to(jnp.exp2(TOP - exponent) * factor, (CIN, COUT))
    for x in range(XS):
        sent_ref[x, XROWS : XROWS + XMARKS, :] = jnp.broadcast_to(exponent, (XMARKS, COUT))
    for tap in range(TAPS):
        u, v, w = tap // 9, tap // 3 % 3, tap % 3
        block = taps[u][v * CIN : (v + 1) * CIN, w * COUT : (w + 1) * COUT] * scale
        first = tap * CIN
        while first < (tap + 1) * CIN:
            x = first // XROWS
            last = min((tap + 1) * CIN, (x + 1) * XROWS)
            sent_ref[x, first - x * XROWS : last - x * XROWS, :] = block[first - tap * CIN : last - tap * CIN]
            first = last


def grad_kernel(act_ref, high_ref, moved_ref, sum_ref, up_ref, down_ref, gin_ref, wide, acts, grads):
    spread(high_ref, wide, grads, 0)
    sums = by_cells(down_ref, grads) + by_cells(up_ref, moved_ref) + sum_ref[...]
    for y in range(YC):
        total = sums[CIN : 2 * CIN, y * ZC : (y + 1) * ZC]
        if y + 1 < YC:
            total = total + sums[0:CIN, (y + 1) * ZC : (y + 2) * ZC]
        if y - 1 >= 0:
            total = total + sums[2 * CIN : 3 * CIN, (y - 1) * ZC : y * ZC]
        acts[pl.ds(y, CIN, stride=YC), :] = total
    grad_hidden = acts[...].reshape(CIN, YC, ZC)
    act = act_ref[...].astype(jnp.float32)
    gin_ref[...] = (grad_hidden * jnp.where(act > 0, 1.0, slope)).astype(jnp.bfloat16)


def after_x_kernel(got_ref, sent_ref, total):
    exps = [got_ref[i, XROWS : XROWS + 1, :] for i in range(XS)]
    largest = functools.reduce(jnp.maximum, exps) + 2.0
    total[...] = sum(got_ref[i, 0:XROWS, :] * jnp.exp2(exps[i] - largest) for i in range(XS))
    for part in range(YCS):
        row = 9 * (part // 4) + 2 * (part % 4)
        for i in range(PART):
            sent_ref[part, i * ZS : (i + 1) * ZS, :] = total[pl.ds(row + i, ZS, stride=ZROWS), :]
        sent_ref[part, PART * ZS : PART * ZS + YMARKS, :] = jnp.broadcast_to(largest, (YMARKS, COUT))


def after_y_kernel(got_ref, sent_ref):
    total = jnp.zeros((PART * ZS, COUT), jnp.float32)
    for i in range(YCS):
        weight = jnp.exp2(got_ref[i, PART * ZS : PART * ZS + 1, :] - TOP)
        total = total + got_ref[i, 0 : PART * ZS, :] * weight
    for i in range(PART):
        sent_ref[:, i, :] = total[i * ZS : (i + 1) * ZS]


def call(body, name, outs, scratch, flops, *args):
    vmem = pl.BlockSpec(memory_space=pltpu.VMEM)
    return pl.pallas_call(
        body,
        out_shape=tuple(jax.ShapeDtypeStruct(shape, dtype) for shape, dtype in outs),
        in_specs=[vmem] * len(args),
        out_specs=tuple([vmem] * len(outs)),
        scratch_shapes=[pltpu.VMEM(shape, dtype) for shape, dtype in scratch],
        compiler_params=pltpu.CompilerParams(vmem_limit_bytes=16 * 1024 * 1024),
        cost_estimate=pl.CostEstimate(flops=flops, bytes_accessed=2_000_000, transcendentals=0),
        name=name,
    )(*args)


def device(x, zl, zh, y, c):
    return (x * ZL + zl) * ZH * YCS + zh * YCS + y * CS + c


def groups():
    along_x = [[x * ZL + zl for x in range(XS)] for zl in range(ZL)]
    along_y = [[zh * YCS + i for i in range(YCS)] for zh in range(ZH)]
    along_z = [
        [device(x, zl, zh, y, c) for zl in range(ZL) for zh in range(ZH)]
        for x in range(XS)
        for y in range(YS)
        for c in range(CS)
    ]
    return along_x, along_y, along_z


def exchanged(x, axis, members):
    return lax.all_to_all(x, axis, 0, 0, tiled=True, axis_index_groups=members)


def on_device(pre_act, grad_out, weight):
    f32, bf16, f16 = jnp.float32, jnp.bfloat16, jnp.float16
    count = pre_act.shape[0] * lax.axis_size("batch") * lax.axis_size("space") * CELLS
    factor = float(1.0 / count**0.5)
    steps = lax.axis_size("space")
    forward = [(i, i + 1) for i in range(steps - 1)]
    backward = [(i + 1, i) for i in range(steps - 1)]
    along_x, along_y, along_z = groups()

    act = pre_act.reshape(CIN, YC, ZC)
    own = grad_out.reshape(COUT, YC, ZC)
    low = lax.ppermute(own, "space", forward)
    low_act = lax.ppermute(act, "space", forward)
    plane = ((COUT * YC, ZC), f32)
    small = ((CIN * YC, ZC), f32)
    stacked, moved, third = ((3 * CIN, CELLS), bf16), ((3 * COUT, CELLS), bf16), ((3 * CIN, 3 * COUT), bf16)
    hids, grads, taps, sums, up, down = call(
        own_kernel,
        "own_plane",
        [stacked, moved, ((3 * CIN, 3 * COUT), f32), ((3 * CIN, CELLS), f32), third, third],
        [plane, small, third],
        1_000_000_000,
        act, own, weight,
    )
    sent, low_grads = call(
        functools.partial(side_kernel, factor),
        "side_planes",
        [((XS, XROWS + XMARKS, COUT), f32), moved],
        [plane, small, stacked],
        1_000_000_000,
        low_act, low, hids, grads, taps,
    )
    got = exchanged(sent.astype(f16), "space", along_x).astype(f32)
    (sent,) = call(
        after_x_kernel, "after_x", [((YCS, PART * ZS + YMARKS, COUT), f32)], [((XROWS, COUT), f32)], 1_000_000, got
    )
    own, sent = lax.optimization_barrier((own, sent))
    high = lax.ppermute(own, "space", backward)
    got = exchanged(sent.astype(f16), "batch", along_y).astype(f32)
    (sent,) = call(after_y_kernel, "after_y", [((ZS, PART, COUT), f32)], [], 1_000_000, got)
    sums, _ = lax.optimization_barrier((sums, sent))
    (grad_in,) = call(
        grad_kernel,
        "grad_planes",
        [((CIN, YC, ZC), bf16)],
        [plane, small, moved],
        2_000_000_000,
        act, high, low_grads, sums, up, down,
    )
    got = exchanged(sent, ("space", "batch"), along_z)
    total = jnp.sum(got, axis=0).reshape(-1)
    start = (lax.axis_index("batch") & 3) * 32
    weight_grad = lax.dynamic_slice(total, (start,), (ROWS * COUT // 768,))
    return (grad_in.reshape(pre_act.shape), weight_grad)


def solution(mesh):
    return jax.shard_map(
        on_device,
        mesh=mesh,
        in_specs=(
            P("batch", None, "space", None, None),
            P("batch", None, "space", None, None),
            P(),
        ),
        out_specs=(P("batch", None, "space", None, None), P(("space", "batch"))),
        check_vma=False,
    )
```

```python
import functools

import jax
import jax.numpy as jnp
from jax import lax
from jax.experimental import pallas as pl
from jax.experimental.pallas import tpu as pltpu
from jax.sharding import PartitionSpec as P

slope = 0.3
CIN, COUT, YC, ZC, TAPS = 64, 128, 8, 128, 27
CELLS = YC * ZC
ROWS = TAPS * CIN
XS, ZL, ZH, YS, CS = 4, 6, 2, 8, 2
ZS, YCS = ZL * ZH, YS * CS
XROWS = ROWS // XS
ZROWS = XROWS // ZS
PART = 3
XMARKS, YMARKS = 8, 4
TOP = 12.0


def shifted_lanes(tile, by):
    lane = lax.broadcasted_iota(jnp.int32, tile.shape, 1)
    if by > 0:
        return jnp.where(lane > 0, pltpu.roll(tile, 1, 1), 0.0)
    return jnp.where(lane < ZC - 1, pltpu.roll(tile, ZC - 1, 1), 0.0)


def spread(ref, wide, grads, first):
    wide[...] = ref[...].astype(jnp.float32).reshape(COUT * YC, ZC)
    for y in range(YC):
        tile = wide[pl.ds(y, COUT, stride=YC), :]
        for w in (-1, 0, 1):
            moved = tile if w == 0 else shifted_lanes(tile, w)
            row = first + (w + 1) * COUT
            grads[row : row + COUT, y * ZC : (y + 1) * ZC] = moved.astype(jnp.bfloat16)


def by_taps(hids, grads):
    return lax.dot_general(
        hids[...], grads[...], (((1,), (1,)), ((), ())), preferred_element_type=jnp.float32
    )


def by_cells(weights, grads):
    return lax.dot_general(
        weights[...], grads[...], (((1,), (0,)), ((), ())), preferred_element_type=jnp.float32
    )


def stack_hidden(act, acts, hids):
    hidden = jnp.where(act > 0, act, slope * act).astype(jnp.bfloat16)
    acts[...] = hidden.astype(jnp.float32).reshape(CIN * YC, ZC)
    for y in range(YC):
        tile = acts[pl.ds(y, CIN, stride=YC), :].astype(jnp.bfloat16)
        for v in (-1, 0, 1):
            if 0 <= y - v < YC:
                hids[(v + 1) * CIN : (v + 2) * CIN, (y - v) * ZC : (y - v + 1) * ZC] = tile
    none = jnp.zeros((CIN, ZC), jnp.bfloat16)
    hids[0:CIN, 0:ZC] = none
    hids[2 * CIN : 3 * CIN, (YC - 1) * ZC : YC * ZC] = none


def own_kernel(
    act_ref, own_ref, w_ref, hid_ref, grad_ref, tap_ref, sum_ref, up_ref, down_ref, kept_ref, wide, acts, mids
):
    kept_ref[...] = own_ref[...]
    spread(own_ref, wide, grad_ref, 0)
    stack_hidden(act_ref[...].astype(jnp.float32), acts, hid_ref)
    for v in range(3):
        for w in range(3):
            rows, lanes = slice(v * CIN, (v + 1) * CIN), slice(w * COUT, (w + 1) * COUT)
            down_ref[rows, lanes] = w_ref[3 * v + w]
            mids[rows, lanes] = w_ref[9 + 3 * v + w]
            up_ref[rows, lanes] = w_ref[18 + 3 * v + w]
    tap_ref[...] = by_taps(hid_ref, grad_ref)
    sum_ref[...] = by_cells(mids, grad_ref)


def side_kernel(
    factor, act_ref, low_ref, hid_ref, grad_ref, tap_ref, sent_ref, moved_ref, wide, acts, hids
):
    spread(low_ref, wide, moved_ref, 0)
    stack_hidden(act_ref[...].astype(jnp.float32), acts, hids)
    taps = (by_taps(hids, grad_ref), tap_ref[...], by_taps(hid_ref, moved_ref))
    most = functools.reduce(jnp.maximum, [jnp.max(jnp.abs(t), keepdims=True) for t in taps])
    exponent = jnp.floor(jnp.log2(jnp.maximum(most * factor, 1e-30))) + 1.0
    scale = jnp.broadcast_to(jnp.exp2(TOP - exponent) * factor, (CIN, COUT))
    for x in range(XS):
        sent_ref[x, XROWS : XROWS + XMARKS, :] = jnp.broadcast_to(exponent, (XMARKS, COUT))
    for tap in range(TAPS):
        u, v, w = tap // 9, tap // 3 % 3, tap % 3
        block = taps[u][v * CIN : (v + 1) * CIN, w * COUT : (w + 1) * COUT] * scale
        first = tap * CIN
        while first < (tap + 1) * CIN:
            x = first // XROWS
            last = min((tap + 1) * CIN, (x + 1) * XROWS)
            sent_ref[x, first - x * XROWS : last - x * XROWS, :] = block[first - tap * CIN : last - tap * CIN]
            first = last


def grad_kernel(act_ref, high_ref, moved_ref, sum_ref, up_ref, down_ref, gin_ref, wide, acts, grads):
    spread(high_ref, wide, grads, 0)
    sums = by_cells(down_ref, grads) + by_cells(up_ref, moved_ref) + sum_ref[...]
    for y in range(YC):
        total = sums[CIN : 2 * CIN, y * ZC : (y + 1) * ZC]
        if y + 1 < YC:
            total = total + sums[0:CIN, (y + 1) * ZC : (y + 2) * ZC]
        if y - 1 >= 0:
            total = total + sums[2 * CIN : 3 * CIN, (y - 1) * ZC : y * ZC]
        acts[pl.ds(y, CIN, stride=YC), :] = total
    grad_hidden = acts[...].reshape(CIN, YC, ZC)
    act = act_ref[...].astype(jnp.float32)
    gin_ref[...] = (grad_hidden * jnp.where(act > 0, 1.0, slope)).astype(jnp.bfloat16)


def after_x_kernel(got_ref, own_ref, sent_ref, copy_ref, total):
    copy_ref[...] = own_ref[...]
    exps = [got_ref[i, XROWS : XROWS + 1, :] for i in range(XS)]
    largest = functools.reduce(jnp.maximum, exps) + 2.0
    total[...] = sum(got_ref[i, 0:XROWS, :] * jnp.exp2(exps[i] - largest) for i in range(XS))
    for part in range(YCS):
        row = 9 * (part // 4) + 2 * (part % 4)
        for i in range(PART):
            sent_ref[part, i * ZS : (i + 1) * ZS, :] = total[pl.ds(row + i, ZS, stride=ZROWS), :]
        sent_ref[part, PART * ZS : PART * ZS + YMARKS, :] = jnp.broadcast_to(largest, (YMARKS, COUT))


def after_y_kernel(got_ref, sent_ref):
    total = jnp.zeros((PART * ZS, COUT), jnp.float32)
    for i in range(YCS):
        weight = jnp.exp2(got_ref[i, PART * ZS : PART * ZS + 1, :] - TOP)
        total = total + got_ref[i, 0 : PART * ZS, :] * weight
    for i in range(PART):
        sent_ref[:, i, :] = total[i * ZS : (i + 1) * ZS]


def call(body, outs, scratch, flops, *args):
    vmem = pl.BlockSpec(memory_space=pltpu.VMEM)
    return pl.pallas_call(
        body,
        out_shape=tuple(jax.ShapeDtypeStruct(shape, dtype) for shape, dtype in outs),
        in_specs=[vmem] * len(args),
        out_specs=tuple([vmem] * len(outs)),
        scratch_shapes=[pltpu.VMEM(shape, dtype) for shape, dtype in scratch],
        compiler_params=pltpu.CompilerParams(vmem_limit_bytes=16 * 1024 * 1024),
        cost_estimate=pl.CostEstimate(flops=flops, bytes_accessed=2_000_000, transcendentals=0),
    )(*args)


def device(x, zl, zh, y, c):
    return (x * ZL + zl) * ZH * YCS + zh * YCS + y * CS + c


def groups():
    along_x = [[x * ZL + zl for x in range(XS)] for zl in range(ZL)]
    along_y = [[zh * YCS + i for i in range(YCS)] for zh in range(ZH)]
    along_z = [
        [device(x, zl, zh, y, c) for zl in range(ZL) for zh in range(ZH)]
        for x in range(XS)
        for y in range(YS)
        for c in range(CS)
    ]
    return along_x, along_y, along_z


def exchanged(x, axis, members):
    return lax.all_to_all(x, axis, 0, 0, tiled=True, axis_index_groups=members)


def gradients(pre_act, grad_out, weight):
    f32, bf16, f16 = jnp.float32, jnp.bfloat16, jnp.float16
    count = pre_act.shape[0] * lax.axis_size("batch") * lax.axis_size("space") * CELLS
    factor = float(1.0 / count**0.5)
    steps = lax.axis_size("space")
    forward = [(i, i + 1) for i in range(steps - 1)]
    backward = [(i + 1, i) for i in range(steps - 1)]
    along_x, along_y, along_z = groups()

    act = pre_act.reshape(CIN, YC, ZC)
    own = grad_out.reshape(COUT, YC, ZC)
    low = lax.ppermute(own, "space", forward)
    low_act = lax.ppermute(act, "space", forward)
    plane = ((COUT * YC, ZC), f32)
    small = ((CIN * YC, ZC), f32)
    stacked, moved, third = ((3 * CIN, CELLS), bf16), ((3 * COUT, CELLS), bf16), ((3 * CIN, 3 * COUT), bf16)
    hids, grads, taps, sums, up, down, kept = call(
        own_kernel,
        [stacked, moved, ((3 * CIN, 3 * COUT), f32), ((3 * CIN, CELLS), f32), third, third, ((COUT, YC, ZC), bf16)],
        [plane, small, third],
        1_000_000_000,
        act, own, weight,
    )
    sent, low_grads = call(
        functools.partial(side_kernel, factor),
        [((XS, XROWS + XMARKS, COUT), f32), moved],
        [plane, small, stacked],
        1_000_000_000,
        low_act, low, hids, grads, taps,
    )
    got = exchanged(sent.astype(f16), "space", along_x).astype(f32)
    sent, own = call(
        after_x_kernel,
        [((YCS, PART * ZS + YMARKS, COUT), f32), ((COUT, YC, ZC), bf16)],
        [((XROWS, COUT), f32)],
        1_000_000,
        got, kept,
    )
    high = lax.ppermute(own, "space", backward)
    got = exchanged(sent.astype(f16), "batch", along_y)
    got = got.astype(f32)
    (sent,) = call(after_y_kernel, [((ZS, PART, COUT), f32)], [], 1_000_000, got)
    sums, _ = lax.optimization_barrier((sums, sent))
    (grad_in,) = call(
        grad_kernel,
        [((CIN, YC, ZC), bf16)],
        [plane, small, moved],
        2_000_000_000,
        act, high, low_grads, sums, up, down,
    )
    got = exchanged(sent, ("space", "batch"), along_z)
    total = jnp.sum(got, axis=0).reshape(-1)
    start = (lax.axis_index("batch") & 3) * 32
    weight_grad = lax.dynamic_slice(total, (start,), (ROWS * COUT // 768,))
    return (grad_in.reshape(pre_act.shape), weight_grad)


def solution(mesh):
    return jax.shard_map(
        gradients,
        mesh=mesh,
        in_specs=(
            P("batch", None, "space", None, None),
            P("batch", None, "space", None, None),
            P(),
        ),
        out_specs=(P("batch", None, "space", None, None), P(("space", "batch"))),
        check_vma=False,
    )
```

```python
import functools

import jax
import jax.numpy as jnp
from jax import lax
from jax.experimental import pallas as pl
from jax.experimental.pallas import tpu as pltpu
from jax.sharding import PartitionSpec as P

slope = 0.3
CIN, COUT, YC, ZC, TAPS = 64, 128, 8, 128, 27
CELLS = YC * ZC
ROWS = TAPS * CIN
XS, ZL, ZH, YS, CS = 4, 6, 2, 8, 2
ZS, YCS = ZL * ZH, YS * CS
XROWS = ROWS // XS
ZROWS = XROWS // ZS
PART = 3
XMARKS, YMARKS = 8, 4
TOP = 12.0


def shifted_lanes(tile, by):
    lane = lax.broadcasted_iota(jnp.int32, tile.shape, 1)
    if by > 0:
        return jnp.where(lane > 0, pltpu.roll(tile, 1, 1), 0.0)
    return jnp.where(lane < ZC - 1, pltpu.roll(tile, ZC - 1, 1), 0.0)


def spread(ref, wide, grads, first):
    wide[...] = ref[...].astype(jnp.float32).reshape(COUT * YC, ZC)
    for y in range(YC):
        tile = wide[pl.ds(y, COUT, stride=YC), :]
        for w in (-1, 0, 1):
            moved = tile if w == 0 else shifted_lanes(tile, w)
            row = first + (w + 1) * COUT
            grads[row : row + COUT, y * ZC : (y + 1) * ZC] = moved.astype(jnp.bfloat16)


def by_taps(hids, grads):
    return lax.dot_general(
        hids[...], grads[...], (((1,), (1,)), ((), ())), preferred_element_type=jnp.float32
    )


def by_cells(weights, grads):
    return lax.dot_general(
        weights[...], grads[...], (((1,), (0,)), ((), ())), preferred_element_type=jnp.float32
    )


def stack_hidden(act, acts, hids):
    hidden = jnp.where(act > 0, act, slope * act).astype(jnp.bfloat16)
    acts[...] = hidden.astype(jnp.float32).reshape(CIN * YC, ZC)
    for y in range(YC):
        tile = acts[pl.ds(y, CIN, stride=YC), :].astype(jnp.bfloat16)
        for v in (-1, 0, 1):
            if 0 <= y - v < YC:
                hids[(v + 1) * CIN : (v + 2) * CIN, (y - v) * ZC : (y - v + 1) * ZC] = tile
    none = jnp.zeros((CIN, ZC), jnp.bfloat16)
    hids[0:CIN, 0:ZC] = none
    hids[2 * CIN : 3 * CIN, (YC - 1) * ZC : YC * ZC] = none


def own_kernel(
    act_ref, own_ref, w_ref, hid_ref, grad_ref, tap_ref, sum_ref, up_ref, down_ref, kept_ref, wide, acts, mids
):
    kept_ref[...] = own_ref[...]
    spread(own_ref, wide, grad_ref, 0)
    stack_hidden(act_ref[...].astype(jnp.float32), acts, hid_ref)
    for v in range(3):
        for w in range(3):
            rows, lanes = slice(v * CIN, (v + 1) * CIN), slice(w * COUT, (w + 1) * COUT)
            down_ref[rows, lanes] = w_ref[3 * v + w]
            mids[rows, lanes] = w_ref[9 + 3 * v + w]
            up_ref[rows, lanes] = w_ref[18 + 3 * v + w]
    tap_ref[...] = by_taps(hid_ref, grad_ref)
    sum_ref[...] = by_cells(mids, grad_ref)


def side_kernel(
    factor, act_ref, low_ref, hid_ref, grad_ref, tap_ref, sent_ref, moved_ref, wide, acts, hids
):
    spread(low_ref, wide, moved_ref, 0)
    stack_hidden(act_ref[...].astype(jnp.float32), acts, hids)
    taps = (by_taps(hids, grad_ref), tap_ref[...], by_taps(hid_ref, moved_ref))
    most = functools.reduce(jnp.maximum, [jnp.max(jnp.abs(t), keepdims=True) for t in taps])
    exponent = jnp.floor(jnp.log2(jnp.maximum(most * factor, 1e-30))) + 1.0
    scale = jnp.broadcast_to(jnp.exp2(TOP - exponent) * factor, (CIN, COUT))
    for x in range(XS):
        sent_ref[x, XROWS : XROWS + XMARKS, :] = jnp.broadcast_to(exponent, (XMARKS, COUT))
    for tap in range(TAPS):
        u, v, w = tap // 9, tap // 3 % 3, tap % 3
        block = taps[u][v * CIN : (v + 1) * CIN, w * COUT : (w + 1) * COUT] * scale
        first = tap * CIN
        while first < (tap + 1) * CIN:
            x = first // XROWS
            last = min((tap + 1) * CIN, (x + 1) * XROWS)
            sent_ref[x, first - x * XROWS : last - x * XROWS, :] = block[first - tap * CIN : last - tap * CIN]
            first = last


def grad_kernel(act_ref, high_ref, moved_ref, sum_ref, up_ref, down_ref, gin_ref, wide, acts, grads):
    spread(high_ref, wide, grads, 0)
    sums = by_cells(down_ref, grads) + by_cells(up_ref, moved_ref) + sum_ref[...]
    for y in range(YC):
        total = sums[CIN : 2 * CIN, y * ZC : (y + 1) * ZC]
        if y + 1 < YC:
            total = total + sums[0:CIN, (y + 1) * ZC : (y + 2) * ZC]
        if y - 1 >= 0:
            total = total + sums[2 * CIN : 3 * CIN, (y - 1) * ZC : y * ZC]
        acts[pl.ds(y, CIN, stride=YC), :] = total
    grad_hidden = acts[...].reshape(CIN, YC, ZC)
    act = act_ref[...].astype(jnp.float32)
    gin_ref[...] = (grad_hidden * jnp.where(act > 0, 1.0, slope)).astype(jnp.bfloat16)


def keep_kernel(own_ref, kept_ref):
    kept_ref[...] = own_ref[...]


def after_x_kernel(got_ref, sent_ref, total):
    exps = [got_ref[i, XROWS : XROWS + 1, :] for i in range(XS)]
    largest = functools.reduce(jnp.maximum, exps) + 2.0
    total[...] = sum(got_ref[i, 0:XROWS, :] * jnp.exp2(exps[i] - largest) for i in range(XS))
    for part in range(YCS):
        row = 9 * (part // 4) + 2 * (part % 4)
        for i in range(PART):
            sent_ref[part, i * ZS : (i + 1) * ZS, :] = total[pl.ds(row + i, ZS, stride=ZROWS), :]
        sent_ref[part, PART * ZS : PART * ZS + YMARKS, :] = jnp.broadcast_to(largest, (YMARKS, COUT))


def after_y_kernel(got_ref, sent_ref):
    total = jnp.zeros((PART * ZS, COUT), jnp.float32)
    for i in range(YCS):
        weight = jnp.exp2(got_ref[i, PART * ZS : PART * ZS + 1, :] - TOP)
        total = total + got_ref[i, 0 : PART * ZS, :] * weight
    for i in range(PART):
        sent_ref[:, i, :] = total[i * ZS : (i + 1) * ZS]


def call(body, outs, scratch, flops, *args):
    vmem = pl.BlockSpec(memory_space=pltpu.VMEM)
    return pl.pallas_call(
        body,
        out_shape=tuple(jax.ShapeDtypeStruct(shape, dtype) for shape, dtype in outs),
        in_specs=[vmem] * len(args),
        out_specs=tuple([vmem] * len(outs)),
        scratch_shapes=[pltpu.VMEM(shape, dtype) for shape, dtype in scratch],
        compiler_params=pltpu.CompilerParams(vmem_limit_bytes=16 * 1024 * 1024),
        cost_estimate=pl.CostEstimate(flops=flops, bytes_accessed=2_000_000, transcendentals=0),
    )(*args)


def device(x, zl, zh, y, c):
    return (x * ZL + zl) * ZH * YCS + zh * YCS + y * CS + c


def groups():
    along_x = [[x * ZL + zl for x in range(XS)] for zl in range(ZL)]
    along_y = [[zh * YCS + i for i in range(YCS)] for zh in range(ZH)]
    along_z = [
        [device(x, zl, zh, y, c) for zl in range(ZL) for zh in range(ZH)]
        for x in range(XS)
        for y in range(YS)
        for c in range(CS)
    ]
    return along_x, along_y, along_z


def exchanged(x, axis, members):
    return lax.all_to_all(x, axis, 0, 0, tiled=True, axis_index_groups=members)


def gradients(pre_act, grad_out, weight):
    f32, bf16, f16 = jnp.float32, jnp.bfloat16, jnp.float16
    count = pre_act.shape[0] * lax.axis_size("batch") * lax.axis_size("space") * CELLS
    factor = float(1.0 / count**0.5)
    steps = lax.axis_size("space")
    forward = [(i, i + 1) for i in range(steps - 1)]
    backward = [(i + 1, i) for i in range(steps - 1)]
    along_x, along_y, along_z = groups()

    act = pre_act.reshape(CIN, YC, ZC)
    own = grad_out.reshape(COUT, YC, ZC)
    low = lax.ppermute(own, "space", forward)
    low_act = lax.ppermute(act, "space", forward)
    plane = ((COUT * YC, ZC), f32)
    small = ((CIN * YC, ZC), f32)
    stacked, moved, third = ((3 * CIN, CELLS), bf16), ((3 * COUT, CELLS), bf16), ((3 * CIN, 3 * COUT), bf16)
    hids, grads, taps, sums, up, down, kept = call(
        own_kernel,
        [stacked, moved, ((3 * CIN, 3 * COUT), f32), ((3 * CIN, CELLS), f32), third, third, ((COUT, YC, ZC), bf16)],
        [plane, small, third],
        1_000_000_000,
        act, own, weight,
    )
    start = (lax.axis_index("batch") & 3) * 32
    start, taps = lax.optimization_barrier((start, taps))
    sent, low_grads = call(
        functools.partial(side_kernel, factor),
        [((XS, XROWS + XMARKS, COUT), f32), moved],
        [plane, small, stacked],
        1_000_000_000,
        low_act, low, hids, grads, taps,
    )
    got = exchanged(sent.astype(f16), "space", along_x)
    got = got.astype(f32)
    (own,) = call(keep_kernel, [((COUT, YC, ZC), bf16)], [], 1_000_000, kept)
    high = lax.ppermute(own, "space", backward)
    (sent,) = call(after_x_kernel, [((YCS, PART * ZS + YMARKS, COUT), f32)], [((XROWS, COUT), f32)], 1_000_000, got)
    got = exchanged(sent.astype(f16), "batch", along_y).astype(f32)
    (sent,) = call(after_y_kernel, [((ZS, PART, COUT), f32)], [], 1_000_000, got)
    sums, _ = lax.optimization_barrier((sums, sent))
    (grad_in,) = call(
        grad_kernel,
        [((CIN, YC, ZC), bf16)],
        [plane, small, moved],
        2_000_000_000,
        act, high, low_grads, sums, up, down,
    )
    got = exchanged(sent, ("space", "batch"), along_z)
    total = jnp.sum(got, axis=0).reshape(-1)
    weight_grad = lax.dynamic_slice(total, (start,), (ROWS * COUT // 768,))
    return (grad_in.reshape(pre_act.shape), weight_grad)


def solution(mesh):
    return jax.shard_map(
        gradients,
        mesh=mesh,
        in_specs=(
            P("batch", None, "space", None, None),
            P("batch", None, "space", None, None),
            P(),
        ),
        out_specs=(P("batch", None, "space", None, None), P(("space", "batch"))),
        check_vma=False,
    )
```

```python
import functools

import jax
import jax.numpy as jnp
from jax import lax
from jax.experimental import pallas as pl
from jax.experimental.pallas import tpu as pltpu
from jax.sharding import PartitionSpec as P


slope = 0.3
CIN, COUT, YC, ZC, TAPS = 64, 128, 8, 128, 27
CELLS = YC * ZC
ROWS = TAPS * CIN
XS, ZL, ZH, YS, CS = 4, 6, 2, 8, 2
ZS, YCS = ZL * ZH, YS * CS
XROWS = ROWS // XS
ZROWS = XROWS // ZS
PART = 3
XMARKS, YMARKS = 8, 4
TOP = 12.0


def shifted_lanes(tile, by):
    lane = lax.broadcasted_iota(jnp.int32, tile.shape, 1)
    if by > 0:
        return jnp.where(lane > 0, pltpu.roll(tile, 1, 1), 0.0)
    return jnp.where(lane < ZC - 1, pltpu.roll(tile, ZC - 1, 1), 0.0)


def spread(ref, wide, grads, first):
    wide[...] = ref[...].astype(jnp.float32).reshape(COUT * YC, ZC)
    for y in range(YC):
        tile = wide[pl.ds(y, COUT, stride=YC), :]
        for w in (-1, 0, 1):
            moved = tile if w == 0 else shifted_lanes(tile, w)
            row = first + (w + 1) * COUT
            grads[row : row + COUT, y * ZC : (y + 1) * ZC] = moved.astype(jnp.bfloat16)


def by_taps(hids, grads):
    return lax.dot_general(
        hids[...], grads[...], (((1,), (1,)), ((), ())), preferred_element_type=jnp.float32
    )


def by_cells(weights, grads):
    return lax.dot_general(
        weights[...], grads[...], (((1,), (0,)), ((), ())), preferred_element_type=jnp.float32
    )


def stack_hidden(act, acts, hids):
    hidden = jnp.where(act > 0, act, slope * act).astype(jnp.bfloat16)
    acts[...] = hidden.astype(jnp.float32).reshape(CIN * YC, ZC)
    for y in range(YC):
        tile = acts[pl.ds(y, CIN, stride=YC), :].astype(jnp.bfloat16)
        for v in (-1, 0, 1):
            if 0 <= y - v < YC:
                hids[(v + 1) * CIN : (v + 2) * CIN, (y - v) * ZC : (y - v + 1) * ZC] = tile
    none = jnp.zeros((CIN, ZC), jnp.bfloat16)
    hids[0:CIN, 0:ZC] = none
    hids[2 * CIN : 3 * CIN, (YC - 1) * ZC : YC * ZC] = none


def own_kernel(
    act_hbm, own_hbm, w_hbm, grad_ref, tap_ref, sum_ref, up_ref, down_ref, act_ref, own_ref, w_ref, wide, acts, hids, mids, sems
):
    pairs = ((own_hbm, own_ref), (act_hbm, act_ref), (w_hbm, w_ref))
    copies = [pltpu.make_async_copy(a, b, sems.at[i]) for i, (a, b) in enumerate(pairs)]
    for copy in copies:
        copy.start()
    copies[0].wait()
    spread(own_ref, wide, grad_ref, 0)
    copies[1].wait()
    stack_hidden(act_ref[...].astype(jnp.float32), acts, hids)
    copies[2].wait()
    for v in range(3):
        for w in range(3):
            rows, lanes = slice(v * CIN, (v + 1) * CIN), slice(w * COUT, (w + 1) * COUT)
            down_ref[rows, lanes] = w_ref[3 * v + w]
            mids[rows, lanes] = w_ref[9 + 3 * v + w]
            up_ref[rows, lanes] = w_ref[18 + 3 * v + w]
    tap_ref[...] = by_taps(hids, grad_ref)
    sum_ref[...] = by_cells(mids, grad_ref)


def chosen(take, swapped, straight):
    return jnp.where(take, swapped[...].astype(jnp.float32), straight[...].astype(jnp.float32))


def side_kernel(
    factor, at_ref, low_ref, high_ref, swap_ref, grad_ref, tap_ref, sent_ref, acts, hids
):
    at = at_ref[0, 0]
    stack_hidden(chosen(at == 0, swap_ref, low_ref), acts, hids)
    below = by_taps(hids, grad_ref)
    stack_hidden(chosen(at == ZL - 1, swap_ref, high_ref), acts, hids)
    above = by_taps(hids, grad_ref)
    taps = (below, tap_ref[...], above)
    most = functools.reduce(jnp.maximum, [jnp.max(jnp.abs(t), keepdims=True) for t in taps])
    exponent = jnp.floor(jnp.log2(jnp.maximum(most * factor, 1e-30))) + 1.0
    scale = jnp.broadcast_to(jnp.exp2(TOP - exponent) * factor, (CIN, COUT))
    for x in range(XS):
        sent_ref[x, XROWS : XROWS + XMARKS, :] = jnp.broadcast_to(exponent, (XMARKS, COUT))
    for tap in range(TAPS):
        u, v, w = tap // 9, tap // 3 % 3, tap % 3
        block = taps[u][v * CIN : (v + 1) * CIN, w * COUT : (w + 1) * COUT] * scale
        first = tap * CIN
        while first < (tap + 1) * CIN:
            x = first // XROWS
            last = min((tap + 1) * CIN, (x + 1) * XROWS)
            sent_ref[x, first - x * XROWS : last - x * XROWS, :] = block[first - tap * CIN : last - tap * CIN]
            first = last


def grad_kernel(
    at_ref, act_ref, low_ref, high_ref, swap_ref, sum_ref, up_ref, down_ref, gin_ref, plane, wide, acts, grads
):
    at = at_ref[0, 0]
    plane[...] = chosen(at == 0, swap_ref, low_ref)
    spread(plane, wide, grads, 0)
    sums = by_cells(up_ref, grads) + sum_ref[...]
    plane[...] = chosen(at == ZL - 1, swap_ref, high_ref)
    spread(plane, wide, grads, 0)
    sums = sums + by_cells(down_ref, grads)
    for y in range(YC):
        total = sums[CIN : 2 * CIN, y * ZC : (y + 1) * ZC]
        if y + 1 < YC:
            total = total + sums[0:CIN, (y + 1) * ZC : (y + 2) * ZC]
        if y - 1 >= 0:
            total = total + sums[2 * CIN : 3 * CIN, (y - 1) * ZC : y * ZC]
        acts[pl.ds(y, CIN, stride=YC), :] = total
    grad_hidden = acts[...].reshape(CIN, YC, ZC)
    act = act_ref[...].astype(jnp.float32)
    gin_ref[...] = (grad_hidden * jnp.where(act > 0, 1.0, slope)).astype(jnp.bfloat16)


def after_x_kernel(got_ref, sent_ref, total):
    exps = [got_ref[i, XROWS : XROWS + 1, :] for i in range(XS)]
    largest = functools.reduce(jnp.maximum, exps) + 2.0
    total[...] = sum(got_ref[i, 0:XROWS, :] * jnp.exp2(exps[i] - largest) for i in range(XS))
    for part in range(YCS):
        row = 9 * (part // 4) + 2 * (part % 4)
        for i in range(PART):
            sent_ref[part, i * ZS : (i + 1) * ZS, :] = total[pl.ds(row + i, ZS, stride=ZROWS), :]
        sent_ref[part, PART * ZS : PART * ZS + YMARKS, :] = jnp.broadcast_to(largest, (YMARKS, COUT))


def after_y_kernel(got_ref, sent_ref):
    total = jnp.zeros((PART * ZS, COUT), jnp.float32)
    for i in range(YCS):
        weight = jnp.exp2(got_ref[i, PART * ZS : PART * ZS + 1, :] - TOP)
        total = total + got_ref[i, 0 : PART * ZS, :] * weight
    for i in range(PART):
        sent_ref[:, i, :] = total[i * ZS : (i + 1) * ZS]


def call(body, outs, scratch, flops, *args, inputs=pltpu.VMEM):
    vmem = pl.BlockSpec(memory_space=pltpu.VMEM)
    given = pl.BlockSpec(memory_space=inputs)
    smem = pl.BlockSpec(memory_space=pltpu.SMEM)
    return pl.pallas_call(
        body,
        out_shape=tuple(jax.ShapeDtypeStruct(shape, dtype) for shape, dtype in outs),
        in_specs=[smem if arg.dtype == jnp.int32 else given for arg in args],
        out_specs=tuple([vmem] * len(outs)),
        scratch_shapes=[pltpu.VMEM(*x) if isinstance(x, tuple) else x for x in scratch],
        compiler_params=pltpu.CompilerParams(vmem_limit_bytes=16 * 1024 * 1024),
        cost_estimate=pl.CostEstimate(flops=flops, bytes_accessed=2_000_000, transcendentals=0),
    )(*args)


def device(x, zl, zh, y, c):
    return (x * ZL + zl) * ZH * YCS + zh * YCS + y * CS + c


def groups():
    along_x = [[x * ZL + zl for x in range(XS)] for zl in range(ZL)]
    along_y = [[zh * YCS + i for i in range(YCS)] for zh in range(ZH)]
    along_z = [
        [device(x, zl, zh, y, c) for zl in range(ZL) for zh in range(ZH)]
        for x in range(XS)
        for y in range(YS)
        for c in range(CS)
    ]
    return along_x, along_y, along_z


def exchanged(x, axis, members):
    return lax.all_to_all(x, axis, 0, 0, tiled=True, axis_index_groups=members)


def sent_along(value, pairs):
    return lax.ppermute(value, "space", pairs)


def gradients(pre_act, grad_out, weight):
    f32, bf16, f16 = jnp.float32, jnp.bfloat16, jnp.float16
    count = pre_act.shape[0] * lax.axis_size("batch") * lax.axis_size("space") * CELLS
    factor = float(1.0 / count**0.5)
    steps = XS * ZL
    forward = [(i, i + 1) for i in range(steps - 1) if (i + 1) % ZL]
    backward = [(target, source) for source, target in forward]
    turns = [(i, i + 1) for i in range(steps - 1) if (i + 1) % ZL == 0]
    turns = turns + [(target, source) for source, target in turns]
    along_x, along_y, along_z = groups()

    act = pre_act.reshape(CIN, YC, ZC)
    own = grad_out.reshape(COUT, YC, ZC)
    swap_act = sent_along(act, turns)
    low_act = sent_along(act, forward)
    high_act = sent_along(act, backward)
    low = sent_along(own, forward)
    plane = ((COUT * YC, ZC), f32)
    small = ((CIN * YC, ZC), f32)
    stacked, moved, third = ((3 * CIN, CELLS), bf16), ((3 * COUT, CELLS), bf16), ((3 * CIN, 3 * COUT), bf16)
    grads, taps, sums, up, down = call(
        own_kernel,
        [moved, ((3 * CIN, 3 * COUT), f32), ((3 * CIN, CELLS), f32), third, third],
        [(act.shape, bf16), (own.shape, bf16), (weight.shape, bf16), plane, small, stacked, third]
        + [pltpu.SemaphoreType.DMA((3,))],
        1_000_000_000,
        *[pltpu.with_memory_space_constraint(x, pltpu.HBM) for x in (act, own, weight)],
        inputs=pltpu.HBM,
    )
    start = (lax.axis_index("batch") & 3) * 32
    at = (lax.axis_index("space") % ZL).astype(jnp.int32).reshape(1, 1)
    start, at, taps = lax.optimization_barrier((start, at, taps))
    (sent,) = call(
        functools.partial(side_kernel, factor),
        [((XS, XROWS + XMARKS, COUT), f32)],
        [small, stacked],
        1_000_000_000,
        at, low_act, high_act, swap_act, grads, taps,
    )
    got = exchanged(sent.astype(f16), "space", along_x).astype(f32)
    (sent,) = call(after_x_kernel, [((YCS, PART * ZS + YMARKS, COUT), f32)], [((XROWS, COUT), f32)], 1_000_000, got)
    own, sent = lax.optimization_barrier((own, sent))
    high = sent_along(own, backward)
    swap_grad = sent_along(own, turns)
    got = exchanged(sent.astype(f16), "batch", along_y).astype(f32)
    (sent,) = call(after_y_kernel, [((ZS, PART, COUT), f32)], [], 1_000_000, got)
    sums, _ = lax.optimization_barrier((sums, sent))
    (grad_in,) = call(
        grad_kernel,
        [((CIN, YC, ZC), bf16)],
        [((COUT, YC, ZC), f32), plane, small, moved],
        2_000_000_000,
        at, act, low, high, swap_grad, sums, up, down,
    )
    got = exchanged(sent, ("space", "batch"), along_z)
    total = jnp.sum(got, axis=0).reshape(-1)
    weight_grad = lax.dynamic_slice(total, (start,), (ROWS * COUT // 768,))
    return (grad_in.reshape(pre_act.shape), weight_grad)


def solution(mesh):
    return jax.shard_map(
        gradients,
        mesh=mesh,
        in_specs=(
            P("batch", None, "space", None, None),
            P("batch", None, "space", None, None),
            P(),
        ),
        out_specs=(P("batch", None, "space", None, None), P(("space", "batch"))),
        check_vma=False,
    )
```

```python
import functools

import jax
import jax.numpy as jnp
from jax import lax
from jax.experimental import pallas as pl
from jax.experimental.pallas import tpu as pltpu
from jax.sharding import PartitionSpec as P


slope = 0.3
CIN, COUT, YC, ZC, TAPS = 64, 128, 8, 128, 27
CELLS = YC * ZC
ROWS = TAPS * CIN
XS, ZL, ZH, YS, CS = 4, 6, 2, 8, 2
ZS, YCS = ZL * ZH, YS * CS
XROWS = ROWS // XS
ZROWS = XROWS // ZS
PART = 3
XMARKS, YMARKS = 8, 4
TOP = 12.0


def shifted_lanes(tile, by):
    lane = lax.broadcasted_iota(jnp.int32, tile.shape, 1)
    if by > 0:
        return jnp.where(lane > 0, pltpu.roll(tile, 1, 1), 0.0)
    return jnp.where(lane < ZC - 1, pltpu.roll(tile, ZC - 1, 1), 0.0)


def spread(ref, wide, grads, first):
    wide[...] = ref[...].astype(jnp.float32).reshape(COUT * YC, ZC)
    for y in range(YC):
        tile = wide[pl.ds(y, COUT, stride=YC), :]
        for w in (-1, 0, 1):
            moved = tile if w == 0 else shifted_lanes(tile, w)
            row = first + (w + 1) * COUT
            grads[row : row + COUT, y * ZC : (y + 1) * ZC] = moved.astype(jnp.bfloat16)


def by_taps(hids, grads):
    return lax.dot_general(
        hids[...], grads[...], (((1,), (1,)), ((), ())), preferred_element_type=jnp.float32
    )


def by_cells(weights, grads):
    return lax.dot_general(
        weights[...], grads[...], (((1,), (0,)), ((), ())), preferred_element_type=jnp.float32
    )


def stack_hidden(act, acts, hids):
    hidden = jnp.where(act > 0, act, slope * act).astype(jnp.bfloat16)
    acts[...] = hidden.astype(jnp.float32).reshape(CIN * YC, ZC)
    for y in range(YC):
        tile = acts[pl.ds(y, CIN, stride=YC), :].astype(jnp.bfloat16)
        for v in (-1, 0, 1):
            if 0 <= y - v < YC:
                hids[(v + 1) * CIN : (v + 2) * CIN, (y - v) * ZC : (y - v + 1) * ZC] = tile
    none = jnp.zeros((CIN, ZC), jnp.bfloat16)
    hids[0:CIN, 0:ZC] = none
    hids[2 * CIN : 3 * CIN, (YC - 1) * ZC : YC * ZC] = none


def own_kernel(act_hbm, own_hbm, grad_ref, tap_ref, act_ref, own_ref, wide, acts, hids, sems):
    pairs = ((own_hbm, own_ref), (act_hbm, act_ref))
    copies = [pltpu.make_async_copy(a, b, sems.at[i]) for i, (a, b) in enumerate(pairs)]
    for copy in copies:
        copy.start()
    copies[0].wait()
    spread(own_ref, wide, grad_ref, 0)
    copies[1].wait()
    stack_hidden(act_ref[...].astype(jnp.float32), acts, hids)
    tap_ref[...] = by_taps(hids, grad_ref)


def chosen(take, swapped, straight):
    return jnp.where(take, swapped[...].astype(jnp.float32), straight[...].astype(jnp.float32))


def side_kernel(
    factor, at_ref, low_ref, high_ref, swap_ref, grad_ref, tap_ref, sent_ref, acts, hids
):
    at = at_ref[0, 0]
    stack_hidden(chosen(at == 0, swap_ref, low_ref), acts, hids)
    below = by_taps(hids, grad_ref)
    stack_hidden(chosen(at == ZL - 1, swap_ref, high_ref), acts, hids)
    above = by_taps(hids, grad_ref)
    taps = (below, tap_ref[...], above)
    most = functools.reduce(jnp.maximum, [jnp.max(jnp.abs(t), keepdims=True) for t in taps])
    exponent = jnp.floor(jnp.log2(jnp.maximum(most * factor, 1e-30))) + 1.0
    scale = jnp.broadcast_to(jnp.exp2(TOP - exponent) * factor, (CIN, COUT))
    for x in range(XS):
        sent_ref[x, XROWS : XROWS + XMARKS, :] = jnp.broadcast_to(exponent, (XMARKS, COUT))
    for tap in range(TAPS):
        u, v, w = tap // 9, tap // 3 % 3, tap % 3
        block = taps[u][v * CIN : (v + 1) * CIN, w * COUT : (w + 1) * COUT] * scale
        first = tap * CIN
        while first < (tap + 1) * CIN:
            x = first // XROWS
            last = min((tap + 1) * CIN, (x + 1) * XROWS)
            sent_ref[x, first - x * XROWS : last - x * XROWS, :] = block[first - tap * CIN : last - tap * CIN]
            first = last


def grad_kernel(
    at_ref, act_ref, own_ref, low_ref, high_ref, swap_ref, w_ref, gin_ref, plane, wide, acts, grads, weights
):
    def part(u, moved):
        for v in range(3):
            for w in range(3):
                rows, lanes = slice(v * CIN, (v + 1) * CIN), slice(w * COUT, (w + 1) * COUT)
                weights[rows, lanes] = w_ref[9 * u + 3 * v + w]
        return by_cells(weights, moved)

    at = at_ref[0, 0]
    sums = part(1, own_ref)
    plane[...] = chosen(at == 0, swap_ref, low_ref)
    spread(plane, wide, grads, 0)
    sums = sums + part(2, grads)
    plane[...] = chosen(at == ZL - 1, swap_ref, high_ref)
    spread(plane, wide, grads, 0)
    sums = sums + part(0, grads)
    for y in range(YC):
        total = sums[CIN : 2 * CIN, y * ZC : (y + 1) * ZC]
        if y + 1 < YC:
            total = total + sums[0:CIN, (y + 1) * ZC : (y + 2) * ZC]
        if y - 1 >= 0:
            total = total + sums[2 * CIN : 3 * CIN, (y - 1) * ZC : y * ZC]
        acts[pl.ds(y, CIN, stride=YC), :] = total
    grad_hidden = acts[...].reshape(CIN, YC, ZC)
    act = act_ref[...].astype(jnp.float32)
    gin_ref[...] = (grad_hidden * jnp.where(act > 0, 1.0, slope)).astype(jnp.bfloat16)


def after_x_kernel(got_ref, sent_ref, total):
    exps = [got_ref[i, XROWS : XROWS + 1, :] for i in range(XS)]
    largest = functools.reduce(jnp.maximum, exps) + 2.0
    total[...] = sum(got_ref[i, 0:XROWS, :] * jnp.exp2(exps[i] - largest) for i in range(XS))
    for part in range(YCS):
        row = 9 * (part // 4) + 2 * (part % 4)
        for i in range(PART):
            sent_ref[part, i * ZS : (i + 1) * ZS, :] = total[pl.ds(row + i, ZS, stride=ZROWS), :]
        sent_ref[part, PART * ZS : PART * ZS + YMARKS, :] = jnp.broadcast_to(largest, (YMARKS, COUT))


def after_y_kernel(got_ref, sent_ref):
    total = jnp.zeros((PART * ZS, COUT), jnp.float32)
    for i in range(YCS):
        weight = jnp.exp2(got_ref[i, PART * ZS : PART * ZS + 1, :] - TOP)
        total = total + got_ref[i, 0 : PART * ZS, :] * weight
    for i in range(PART):
        sent_ref[:, i, :] = total[i * ZS : (i + 1) * ZS]


def call(body, outs, scratch, flops, *args, inputs=pltpu.VMEM):
    vmem = pl.BlockSpec(memory_space=pltpu.VMEM)
    given = pl.BlockSpec(memory_space=inputs)
    smem = pl.BlockSpec(memory_space=pltpu.SMEM)
    return pl.pallas_call(
        body,
        out_shape=tuple(jax.ShapeDtypeStruct(shape, dtype) for shape, dtype in outs),
        in_specs=[smem if arg.dtype == jnp.int32 else given for arg in args],
        out_specs=tuple([vmem] * len(outs)),
        scratch_shapes=[pltpu.VMEM(*x) if isinstance(x, tuple) else x for x in scratch],
        compiler_params=pltpu.CompilerParams(vmem_limit_bytes=16 * 1024 * 1024),
        cost_estimate=pl.CostEstimate(flops=flops, bytes_accessed=2_000_000, transcendentals=0),
    )(*args)


def device(x, zl, zh, y, c):
    return (x * ZL + zl) * ZH * YCS + zh * YCS + y * CS + c


def groups():
    along_x = [[x * ZL + zl for x in range(XS)] for zl in range(ZL)]
    along_y = [[zh * YCS + i for i in range(YCS)] for zh in range(ZH)]
    along_z = [
        [device(x, zl, zh, y, c) for zl in range(ZL) for zh in range(ZH)]
        for x in range(XS)
        for y in range(YS)
        for c in range(CS)
    ]
    return along_x, along_y, along_z


def exchanged(x, axis, members):
    return lax.all_to_all(x, axis, 0, 0, tiled=True, axis_index_groups=members)


def sent_along(value, pairs):
    return lax.ppermute(value, "space", pairs)


def gradients(pre_act, grad_out, weight):
    f32, bf16, f16 = jnp.float32, jnp.bfloat16, jnp.float16
    count = pre_act.shape[0] * lax.axis_size("batch") * lax.axis_size("space") * CELLS
    factor = float(1.0 / count**0.5)
    steps = XS * ZL
    forward = [(i, i + 1) for i in range(steps - 1) if (i + 1) % ZL]
    backward = [(target, source) for source, target in forward]
    turns = [(i, i + 1) for i in range(steps - 1) if (i + 1) % ZL == 0]
    turns = turns + [(target, source) for source, target in turns]
    along_x, along_y, along_z = groups()

    act = pre_act.reshape(CIN, YC, ZC)
    own = grad_out.reshape(COUT, YC, ZC)
    swap_act = sent_along(act, turns)
    low_act = sent_along(act, forward)
    high_act = sent_along(act, backward)
    low = sent_along(own, forward)
    plane = ((COUT * YC, ZC), f32)
    small = ((CIN * YC, ZC), f32)
    stacked, moved, third = ((3 * CIN, CELLS), bf16), ((3 * COUT, CELLS), bf16), ((3 * CIN, 3 * COUT), bf16)
    grads, taps = call(
        own_kernel,
        [moved, ((3 * CIN, 3 * COUT), f32)],
        [(act.shape, bf16), (own.shape, bf16), plane, small, stacked, pltpu.SemaphoreType.DMA((2,))],
        1_000_000_000,
        *[pltpu.with_memory_space_constraint(x, pltpu.HBM) for x in (act, own)],
        inputs=pltpu.HBM,
    )
    start = (lax.axis_index("batch") & 3) * 32
    at = (lax.axis_index("space") % ZL).astype(jnp.int32).reshape(1, 1)
    start, at, taps = lax.optimization_barrier((start, at, taps))
    (sent,) = call(
        functools.partial(side_kernel, factor),
        [((XS, XROWS + XMARKS, COUT), f32)],
        [small, stacked],
        1_000_000_000,
        at, low_act, high_act, swap_act, grads, taps,
    )
    got = exchanged(sent.astype(f16), "space", along_x).astype(f32)
    (sent,) = call(after_x_kernel, [((YCS, PART * ZS + YMARKS, COUT), f32)], [((XROWS, COUT), f32)], 1_000_000, got)
    own, sent = lax.optimization_barrier((own, sent))
    high = sent_along(own, backward)
    swap_grad = sent_along(own, turns)
    got = exchanged(sent.astype(f16), "batch", along_y).astype(f32)
    (sent,) = call(after_y_kernel, [((ZS, PART, COUT), f32)], [], 1_000_000, got)
    grads, _ = lax.optimization_barrier((grads, sent))
    (grad_in,) = call(
        grad_kernel,
        [((CIN, YC, ZC), bf16)],
        [((COUT, YC, ZC), f32), plane, small, moved, third],
        2_000_000_000,
        at, act, grads, low, high, swap_grad, weight,
    )
    got = exchanged(sent, ("space", "batch"), along_z)
    total = jnp.sum(got, axis=0).reshape(-1)
    weight_grad = lax.dynamic_slice(total, (start,), (ROWS * COUT // 768,))
    return (grad_in.reshape(pre_act.shape), weight_grad)


def solution(mesh):
    return jax.shard_map(
        gradients,
        mesh=mesh,
        in_specs=(
            P("batch", None, "space", None, None),
            P("batch", None, "space", None, None),
            P(),
        ),
        out_specs=(P("batch", None, "space", None, None), P(("space", "batch"))),
        check_vma=False,
    )
```

```python
import functools

import jax
import jax.numpy as jnp
from jax import lax
from jax.experimental import pallas as pl
from jax.experimental.pallas import tpu as pltpu
from jax.sharding import PartitionSpec as P


slope = 0.3
CIN, COUT, YC, ZC, TAPS = 64, 128, 8, 128, 27
CELLS = YC * ZC
ROWS = TAPS * CIN
XS, ZL, ZH, YS, CS = 4, 6, 2, 8, 2
ZS, YCS = ZL * ZH, YS * CS
XROWS = ROWS // XS
ZROWS = XROWS // ZS
PART = 3
XMARKS, YMARKS = 8, 4
TOP = 12.0


def shifted_lanes(tile, by):
    lane = lax.broadcasted_iota(jnp.int32, tile.shape, 1)
    if by > 0:
        return jnp.where(lane > 0, pltpu.roll(tile, 1, 1), 0.0)
    return jnp.where(lane < ZC - 1, pltpu.roll(tile, ZC - 1, 1), 0.0)


def spread(ref, wide, grads, first):
    wide[...] = ref[...].astype(jnp.float32).reshape(COUT * YC, ZC)
    for y in range(YC):
        tile = wide[pl.ds(y, COUT, stride=YC), :]
        for w in (-1, 0, 1):
            moved = tile if w == 0 else shifted_lanes(tile, w)
            row = first + (w + 1) * COUT
            grads[row : row + COUT, y * ZC : (y + 1) * ZC] = moved.astype(jnp.bfloat16)


def by_taps(hids, grads):
    return lax.dot_general(
        hids[...], grads[...], (((1,), (1,)), ((), ())), preferred_element_type=jnp.float32
    )


def by_cells(weights, grads):
    return lax.dot_general(
        weights[...], grads[...], (((1,), (0,)), ((), ())), preferred_element_type=jnp.float32
    )


def stack_hidden(act, acts, hids):
    hidden = jnp.where(act > 0, act, slope * act).astype(jnp.bfloat16)
    acts[...] = hidden.astype(jnp.float32).reshape(CIN * YC, ZC)
    for y in range(YC):
        tile = acts[pl.ds(y, CIN, stride=YC), :].astype(jnp.bfloat16)
        for v in (-1, 0, 1):
            if 0 <= y - v < YC:
                hids[(v + 1) * CIN : (v + 2) * CIN, (y - v) * ZC : (y - v + 1) * ZC] = tile
    none = jnp.zeros((CIN, ZC), jnp.bfloat16)
    hids[0:CIN, 0:ZC] = none
    hids[2 * CIN : 3 * CIN, (YC - 1) * ZC : YC * ZC] = none


def own_kernel(act_hbm, own_hbm, grad_ref, tap_ref, kept_ref, act_ref, own_ref, wide, acts, hids, sems):
    pairs = ((own_hbm, own_ref), (act_hbm, act_ref))
    copies = [pltpu.make_async_copy(a, b, sems.at[i]) for i, (a, b) in enumerate(pairs)]
    for copy in copies:
        copy.start()
    copies[0].wait()
    spread(own_ref, wide, grad_ref, 0)
    copies[1].wait()
    stack_hidden(act_ref[...].astype(jnp.float32), acts, hids)
    tap_ref[...] = by_taps(hids, grad_ref)
    kept_ref[...] = own_ref[...]


def keep_kernel(own_ref, kept_ref):
    kept_ref[...] = own_ref[...]


def chosen(take, swapped, straight):
    return jnp.where(take, swapped[...].astype(jnp.float32), straight[...].astype(jnp.float32))


def side_kernel(
    factor, at_ref, low_ref, high_ref, swap_ref, grad_ref, tap_ref, sent_ref, acts, hids
):
    at = at_ref[0, 0]
    stack_hidden(chosen(at == 0, swap_ref, low_ref), acts, hids)
    below = by_taps(hids, grad_ref)
    stack_hidden(chosen(at == ZL - 1, swap_ref, high_ref), acts, hids)
    above = by_taps(hids, grad_ref)
    taps = (below, tap_ref[...], above)
    most = functools.reduce(jnp.maximum, [jnp.max(jnp.abs(t), keepdims=True) for t in taps])
    exponent = jnp.floor(jnp.log2(jnp.maximum(most * factor, 1e-30))) + 1.0
    scale = jnp.broadcast_to(jnp.exp2(TOP - exponent) * factor, (CIN, COUT))
    for x in range(XS):
        sent_ref[x, XROWS : XROWS + XMARKS, :] = jnp.broadcast_to(exponent, (XMARKS, COUT))
    for tap in range(TAPS):
        u, v, w = tap // 9, tap // 3 % 3, tap % 3
        block = taps[u][v * CIN : (v + 1) * CIN, w * COUT : (w + 1) * COUT] * scale
        first = tap * CIN
        while first < (tap + 1) * CIN:
            x = first // XROWS
            last = min((tap + 1) * CIN, (x + 1) * XROWS)
            sent_ref[x, first - x * XROWS : last - x * XROWS, :] = block[first - tap * CIN : last - tap * CIN]
            first = last


def grad_kernel(
    at_ref, act_ref, own_ref, low_ref, high_ref, swap_ref, w_ref, gin_ref, plane, wide, acts, grads, weights
):
    def part(u, moved):
        for v in range(3):
            for w in range(3):
                rows, lanes = slice(v * CIN, (v + 1) * CIN), slice(w * COUT, (w + 1) * COUT)
                weights[rows, lanes] = w_ref[9 * u + 3 * v + w]
        return by_cells(weights, moved)

    at = at_ref[0, 0]
    sums = part(1, own_ref)
    plane[...] = chosen(at == 0, swap_ref, low_ref)
    spread(plane, wide, grads, 0)
    sums = sums + part(2, grads)
    plane[...] = chosen(at == ZL - 1, swap_ref, high_ref)
    spread(plane, wide, grads, 0)
    sums = sums + part(0, grads)
    for y in range(YC):
        total = sums[CIN : 2 * CIN, y * ZC : (y + 1) * ZC]
        if y + 1 < YC:
            total = total + sums[0:CIN, (y + 1) * ZC : (y + 2) * ZC]
        if y - 1 >= 0:
            total = total + sums[2 * CIN : 3 * CIN, (y - 1) * ZC : y * ZC]
        acts[pl.ds(y, CIN, stride=YC), :] = total
    grad_hidden = acts[...].reshape(CIN, YC, ZC)
    act = act_ref[...].astype(jnp.float32)
    gin_ref[...] = (grad_hidden * jnp.where(act > 0, 1.0, slope)).astype(jnp.bfloat16)


def after_x_kernel(got_ref, sent_ref, total):
    exps = [got_ref[i, XROWS : XROWS + 1, :] for i in range(XS)]
    largest = functools.reduce(jnp.maximum, exps) + 2.0
    total[...] = sum(got_ref[i, 0:XROWS, :] * jnp.exp2(exps[i] - largest) for i in range(XS))
    for part in range(YCS):
        row = 9 * (part // 4) + 2 * (part % 4)
        for i in range(PART):
            sent_ref[part, i * ZS : (i + 1) * ZS, :] = total[pl.ds(row + i, ZS, stride=ZROWS), :]
        sent_ref[part, PART * ZS : PART * ZS + YMARKS, :] = jnp.broadcast_to(largest, (YMARKS, COUT))


def after_y_kernel(got_ref, sent_ref):
    total = jnp.zeros((PART * ZS, COUT), jnp.float32)
    for i in range(YCS):
        weight = jnp.exp2(got_ref[i, PART * ZS : PART * ZS + 1, :] - TOP)
        total = total + got_ref[i, 0 : PART * ZS, :] * weight
    for i in range(PART):
        sent_ref[:, i, :] = total[i * ZS : (i + 1) * ZS]


def call(body, outs, scratch, flops, *args, inputs=pltpu.VMEM):
    vmem = pl.BlockSpec(memory_space=pltpu.VMEM)
    given = pl.BlockSpec(memory_space=inputs)
    smem = pl.BlockSpec(memory_space=pltpu.SMEM)
    return pl.pallas_call(
        body,
        out_shape=tuple(jax.ShapeDtypeStruct(shape, dtype) for shape, dtype in outs),
        in_specs=[smem if arg.dtype == jnp.int32 else given for arg in args],
        out_specs=tuple([vmem] * len(outs)),
        scratch_shapes=[pltpu.VMEM(*x) if isinstance(x, tuple) else x for x in scratch],
        compiler_params=pltpu.CompilerParams(vmem_limit_bytes=16 * 1024 * 1024),
        cost_estimate=pl.CostEstimate(flops=flops, bytes_accessed=2_000_000, transcendentals=0),
    )(*args)


def device(x, zl, zh, y, c):
    return (x * ZL + zl) * ZH * YCS + zh * YCS + y * CS + c


def groups():
    along_x = [[x * ZL + zl for x in range(XS)] for zl in range(ZL)]
    along_y = [[zh * YCS + i for i in range(YCS)] for zh in range(ZH)]
    along_z = [
        [device(x, zl, zh, y, c) for zl in range(ZL) for zh in range(ZH)]
        for x in range(XS)
        for y in range(YS)
        for c in range(CS)
    ]
    return along_x, along_y, along_z


def exchanged(x, axis, members):
    return lax.all_to_all(x, axis, 0, 0, tiled=True, axis_index_groups=members)


def sent_along(value, pairs):
    return lax.ppermute(value, "space", pairs)


def gradients(pre_act, grad_out, weight):
    f32, bf16, f16 = jnp.float32, jnp.bfloat16, jnp.float16
    count = pre_act.shape[0] * lax.axis_size("batch") * lax.axis_size("space") * CELLS
    factor = float(1.0 / count**0.5)
    steps = XS * ZL
    forward = [(i, i + 1) for i in range(steps - 1) if (i + 1) % ZL]
    backward = [(target, source) for source, target in forward]
    turns = [(i, i + 1) for i in range(steps - 1) if (i + 1) % ZL == 0]
    turns = turns + [(target, source) for source, target in turns]
    along_x, along_y, along_z = groups()

    act = pre_act.reshape(CIN, YC, ZC)
    own = grad_out.reshape(COUT, YC, ZC)
    swap_act = sent_along(act, turns)
    low_act = sent_along(act, forward)
    high_act = sent_along(act, backward)
    low = sent_along(own, forward)
    plane = ((COUT * YC, ZC), f32)
    small = ((CIN * YC, ZC), f32)
    stacked, moved, third = ((3 * CIN, CELLS), bf16), ((3 * COUT, CELLS), bf16), ((3 * CIN, 3 * COUT), bf16)
    grads, taps, kept = call(
        own_kernel,
        [moved, ((3 * CIN, 3 * COUT), f32), (own.shape, bf16)],
        [(act.shape, bf16), (own.shape, bf16), plane, small, stacked, pltpu.SemaphoreType.DMA((2,))],
        1_000_000_000,
        *[pltpu.with_memory_space_constraint(x, pltpu.HBM) for x in (act, own)],
        inputs=pltpu.HBM,
    )
    start = (lax.axis_index("batch") & 3) * 32
    at = (lax.axis_index("space") % ZL).astype(jnp.int32).reshape(1, 1)
    start, at, taps = lax.optimization_barrier((start, at, taps))
    (sent,) = call(
        functools.partial(side_kernel, factor),
        [((XS, XROWS + XMARKS, COUT), f32)],
        [small, stacked],
        1_000_000_000,
        at, low_act, high_act, swap_act, grads, taps,
    )
    got = exchanged(sent.astype(f16), "space", along_x)
    (kept,) = call(keep_kernel, [(own.shape, bf16)], [], 1_000_000, kept)
    swap_grad = sent_along(kept, turns)
    (sent,) = call(
        after_x_kernel, [((YCS, PART * ZS + YMARKS, COUT), f32)], [((XROWS, COUT), f32)], 1_000_000, got.astype(f32)
    )
    own, sent = lax.optimization_barrier((own, sent))
    high = sent_along(own, backward)
    got = exchanged(sent.astype(f16), "batch", along_y).astype(f32)
    (sent,) = call(after_y_kernel, [((ZS, PART, COUT), f32)], [], 1_000_000, got)
    grads, _ = lax.optimization_barrier((grads, sent))
    (grad_in,) = call(
        grad_kernel,
        [((CIN, YC, ZC), bf16)],
        [((COUT, YC, ZC), f32), plane, small, moved, third],
        2_000_000_000,
        at, act, grads, low, high, swap_grad, weight,
    )
    got = exchanged(sent, ("space", "batch"), along_z)
    total = jnp.sum(got, axis=0).reshape(-1)
    weight_grad = lax.dynamic_slice(total, (start,), (ROWS * COUT // 768,))
    return (grad_in.reshape(pre_act.shape), weight_grad)


def solution(mesh):
    return jax.shard_map(
        gradients,
        mesh=mesh,
        in_specs=(
            P("batch", None, "space", None, None),
            P("batch", None, "space", None, None),
            P(),
        ),
        out_specs=(P("batch", None, "space", None, None), P(("space", "batch"))),
        check_vma=False,
    )
```
